32 devices in a mesh: py: 4 (over y, x), px: 4 (over z), pz: 2 (over core).
Axes of the slice: x: 2, y: 2, z: 4, core: 2. Of those that a mesh axis runs over, the one named last changes fastest.
Arguments:
- field_now: float32 [16, 512, 64, 128], P('py', 'px', 'pz'), may hold values from 0.5 to 2
- earlier: float32 [16, 512, 64, 128], P('py', 'px', 'pz'), may hold values from 0.2 to 1.8
- speed_square: float32 [16, 512, 64, 128], P('py', 'px', 'pz'), may hold values from 0.05 to 0.3
Outputs:
- anomaly: float32 [16, 512, 64, 128], P('py', 'px', 'pz')
- field_now_end: float32 [16, 512, 64, 128], P('py', 'px', 'pz')
The draws below stay inside these ranges and needn't reach their ends.
All inputs are finite; a program needn't handle non-finite values.
Results may differ from the reference program's by a relative error of at most 0.00002.
Values sent between devices are 32-bit elements; how exact they have to be, the bound alone decides.
A program may use at most 128 MiB of HBM per device.

```python
import jax
import jax.numpy as jnp
from jax import lax

GRID_J = 16
GRID_I = 512
GRID_K = 64
LEVELS = 128
STEPS = 4


def shard_levels(key, extent, pieces, smallest, high):
    factor_of, own = 1.0, jax.random.fold_in(key, 6)
    for dim, blocks in pieces:
        draws = jnp.exp(jax.random.uniform(jax.random.fold_in(own, dim), (blocks,), jnp.float32, smallest / len(pieces), high / len(pieces)))
        factor_of = factor_of * jnp.repeat(draws, extent[dim] // blocks).reshape([-1 if axis == dim else 1 for axis in range(len(extent))])
    return factor_of


def setup_inputs(seed: int = 0) -> dict:
    streams_of = jax.random.split(jax.random.key(seed), 4)
    return {
        "field_now": jnp.clip(0.5 + 1.5 * jax.random.uniform(streams_of[0], (GRID_J, GRID_I, GRID_K, LEVELS), jnp.float32) ** shard_levels(streams_of[0], (GRID_J, GRID_I, GRID_K, LEVELS), ((0, 4), (1, 4), (2, 2)), -0.2, 0.2), 0.5, 2.0),
        "earlier": jnp.clip(0.2 + 1.5999999 * jax.random.uniform(streams_of[1], (GRID_J, GRID_I, GRID_K, LEVELS), jnp.float32) ** shard_levels(streams_of[1], (GRID_J, GRID_I, GRID_K, LEVELS), ((0, 4), (1, 4), (2, 2)), -0.2, 0.2), 0.2, 1.8),
        "speed_square": jnp.clip(0.05 + 0.25 * jax.random.uniform(streams_of[2], (GRID_J, GRID_I, GRID_K, LEVELS), jnp.float32) ** shard_levels(streams_of[2], (GRID_J, GRID_I, GRID_K, LEVELS), ((0, 4), (1, 4), (2, 2)), -0.2, 0.2), 0.05, 0.3),
    }


def inner_cells(values, dims):
    for dim in dims:
        values = lax.slice_in_dim(values, 1, values.shape[dim] - 1, axis=dim)
    return values

def side_cells(values, dim, start, dims):
    others = [other for other in dims if other != dim]
    values = inner_cells(values, others)
    return lax.slice_in_dim(values, start, start + values.shape[dim] - 2, axis=dim)

def advance(padded, before, speed_square):
    middle = inner_cells(padded, (0, 1, 2))
    lower = [side_cells(padded, dim, 0, (0, 1, 2)) for dim in (0, 1, 2)]
    upper = [side_cells(padded, dim, 2, (0, 1, 2)) for dim in (0, 1, 2)]
    spread = lower[0] + upper[0] + lower[1] + upper[1] + lower[2] + upper[2] - 6.0 * middle
    return 2.0 * middle - before + speed_square * spread

def reference(field_now, earlier, speed_square):
    for step in range(STEPS):
        later = advance(jnp.pad(field_now, ((1, 1), (1, 1), (1, 1), (0, 0)), mode='constant'), earlier, speed_square)
        earlier, field_now = (field_now, later)
    line_mean = lax.optimization_barrier(jnp.mean(field_now, axis=1, keepdims=True))
    centred = field_now - line_mean
    line_variance = lax.optimization_barrier(jnp.mean(centred * centred, axis=1, keepdims=True))
    anomaly = centred * lax.rsqrt(line_variance + 0.0001)
    return (anomaly, field_now)
```

```python
import functools

import jax
import jax.numpy as jnp
from jax import lax
from jax.experimental import pallas as pl
from jax.experimental.pallas import tpu as pltpu
from jax.sharding import PartitionSpec as P

STEPS = 4
PAD = 8
LIMIT = 54 * 2**20
MESH = pl.DeviceIdType.MESH


def relays(mesh):
    devices = mesh.devices
    line = [devices[(n,) + (0,) * (devices.ndim - 1)] for n in range(devices.shape[0])]
    places = [getattr(device, "coords", None) for device in line]
    if any(place is None for place in places):
        return ()
    places = [tuple(place) for place in places]
    jobs = []
    for low in range(len(line) - 1):
        for a, b in ((low, low + 1), (low + 1, low)):
            turn = (places[a][0],) + places[b][1:]
            if turn in places and turn not in (places[a], places[b]):
                jobs.append((a, b, places.index(turn)))
    return tuple(jobs)


def steps_kernel(jobs, pieces, axes, f_ref, e_ref, c_ref, far, mean_out, scale_out,
                 field, speed, halo, relay, stat_in, stat_edge, load_sem, py_send, py_recv,
                 r_send, r_recv, side_send, side_recv, st_send, st_recv):
    planes, lines, depth, levels = c_ref.shape
    tiles = depth // PAD
    chunks = tiles * pieces
    rows = lines // pieces
    edges = sorted({0, planes - 1})
    inner = pl.ds(PAD, depth)
    me = {name: lax.axis_index(name) for name in axes}
    count = {name: axes[name] for name in axes}
    py = me["py"]

    barrier = pltpu.get_barrier_semaphore()
    greeted = 0
    for name in axes:
        for n in range(1, count[name]):
            pl.semaphore_signal(
                barrier, inc=1, device_id={name: lax.rem(me[name] + n, count[name])},
                device_id_type=MESH,
            )
            greeted += 1
    pl.semaphore_wait(barrier, greeted)

    def there(name, way):
        return me[name] < count[name] - 1 if way else me[name] > 0

    def done(ref, sem):
        pltpu.make_async_copy(ref, ref, sem).wait()

    def part(c, line, cell):
        start = cell + (c // pieces) * PAD
        if cell % PAD == 0:
            start = pl.multiple_of(start, PAD)
        return pl.ds(line + (c % pieces) * rows, rows), pl.ds(start, PAD)

    def edge(step, c, way):
        plane = planes - 1 if way else 0
        if step == 0:
            return f_ref.at[(plane,) + part(c, 0, 0)]
        return field.at[(step % 2, plane) + part(c, 1, PAD)]

    def landing(step, c, side):
        return halo.at[(side, step % 2) + part(c, 0, 0)]

    def send_py(step, c):
        for way in (0, 1):
            beyond = py + (2 * way - 1)
            direct = there("py", way)
            for slot, (a, b, via) in enumerate(jobs):
                if b - a != 2 * way - 1:
                    continue
                turned = jnp.logical_and(py == a, c % 2 == 0)
                direct = jnp.logical_and(direct, jnp.logical_not(turned))

                @pl.when(turned)
                def _(slot=slot, via=via, way=way):
                    pltpu.make_async_remote_copy(
                        src_ref=edge(step, c, way),
                        dst_ref=relay.at[job_slot(slot), step, c // 2],
                        send_sem=py_send.at[way, step % 2, c],
                        recv_sem=r_recv.at[job_slot(slot), step, c // 2],
                        device_id={"py": via}, device_id_type=MESH,
                    ).start()

            @pl.when(direct)
            def _(way=way, beyond=beyond):
                pltpu.make_async_remote_copy(
                    src_ref=edge(step, c, way),
                    dst_ref=landing(step, c, 1 - way),
                    send_sem=py_send.at[way, step % 2, c],
                    recv_sem=py_recv.at[1 - way, step % 2, c],
                    device_id={"py": beyond}, device_id_type=MESH,
                ).start()

    def job_slot(slot):
        return [via for _, _, via in jobs[:slot]].count(jobs[slot][2])

    def forward(step, c):
        for slot, (a, b, via) in enumerate(jobs):
            @pl.when(py == via)
            def _(slot=slot, a=a, b=b):
                way = 1 if b > a else 0
                held = relay.at[job_slot(slot), step, c // 2]
                done(held, r_recv.at[job_slot(slot), step, c // 2])
                pltpu.make_async_remote_copy(
                    src_ref=held,
                    dst_ref=landing(step, c, 1 - way),
                    send_sem=r_send.at[job_slot(slot), step, c // 2],
                    recv_sem=py_recv.at[1 - way, step % 2, c],
                    device_id={"py": b}, device_id_type=MESH,
                ).start()

    def forward_late(step, c):
        if jobs:
            @pl.when(c % 2 == 1)
            def _():
                forward(step, c - 1)

    def sent_py(step, c):
        for way in (0, 1):
            @pl.when(there("py", way))
            def _(way=way):
                done(edge(step, c, way), py_send.at[way, step % 2, c])

    def arrived_py(step, c):
        for side in (0, 1):
            @pl.when(there("py", side))
            def _(side=side):
                done(landing(step, c, side), py_recv.at[side, step % 2, c])

    def side_source(step, name, way):
        if name == "px":
            at = lines - 1 if way else 0
            if step == 0:
                return f_ref.at[:, pl.ds(at, 1)]
            return field.at[step % 2, :, pl.ds(1 + at, 1), inner]
        at = depth - PAD if way else 0
        if step == 0:
            return f_ref.at[:, :, pl.ds(at, PAD)]
        return field.at[step % 2, :, pl.ds(1, lines), pl.ds(PAD + at, PAD)]

    def side_landing(slot, name, side):
        if name == "px":
            return field.at[slot, :, pl.ds(lines + 1 if side else 0, 1), inner]
        return field.at[slot, :, pl.ds(1, lines), pl.ds(PAD + depth if side else 0, PAD)]

    def sides(step, what):
        for n, name in enumerate(("px", "pz")):
            for way in (0, 1):
                @pl.when(there(name, way))
                def _(n=n, name=name, way=way):
                    if what == "send":
                        pltpu.make_async_remote_copy(
                            src_ref=side_source(step, name, way),
                            dst_ref=side_landing(step % 2, name, 1 - way),
                            send_sem=side_send.at[n, way, step % 2],
                            recv_sem=side_recv.at[n, 1 - way, step % 2],
                            device_id={name: me[name] + (2 * way - 1)}, device_id_type=MESH,
                        ).start()
                    elif what == "sent":
                        done(side_source(step, name, way), side_send.at[n, way, step % 2])
                    else:
                        done(side_landing(step % 2, name, way), side_recv.at[n, way, step % 2])

    whole = lambda slot: field.at[slot, :, pl.ds(1, lines), inner]
    loads = [
        pltpu.make_async_copy(f_ref, whole(0), load_sem.at[0]),
        pltpu.make_async_copy(e_ref, whole(1), load_sem.at[1]),
        pltpu.make_async_copy(c_ref, speed, load_sem.at[2]),
    ]

    def first(c, _):
        send_py(0, c)
        forward_late(0, c)
        return 0

    lax.fori_loop(0, 2, first, 0)
    sides(0, "send")
    for load in loads:
        load.start()
    lax.fori_loop(2, chunks, first, 0)

    for way in (0, 1):
        @pl.when(jnp.logical_not(there("py", way)))
        def _(way=way):
            def clear(i, _):
                for slot in (0, 1):
                    halo[way, slot, i] = jnp.zeros((depth, levels), jnp.float32)
                return 0
            lax.fori_loop(0, lines, clear, 0)

        @pl.when(jnp.logical_not(there("px", way)))
        def _(way=way):
            for slot in (0, 1):
                for j in range(planes):
                    field[slot, j, lines + 1 if way else 0, inner, :] = jnp.zeros((depth, levels), jnp.float32)

        @pl.when(jnp.logical_not(there("pz", way)))
        def _(way=way):
            def clear(i, _):
                for slot in (0, 1):
                    for j in range(planes):
                        field[slot, j, 1 + i, pl.ds(PAD + depth if way else 0, PAD), :] = jnp.zeros((PAD, levels), jnp.float32)
                return 0
            lax.fori_loop(0, lines, clear, 0)

    for load in loads:
        load.wait()

    px, blocks = me["px"], count["px"]

    def cells(start, tile):
        start = start + tile * PAD
        return pl.ds(pl.multiple_of(start, PAD) if isinstance(start, jax.Array) and start.ndim == 0 else start, PAD)

    def update(step, which, i, tile):
        now, other = step % 2, (step + 1) % 2
        mid, own = cells(PAD, tile), cells(0, tile)
        for j in which:
            here = field[now, j, i + 1, mid, :]
            below = field[now, j - 1, i + 1, mid, :] if j else halo[0, now, i, own, :]
            above = field[now, j + 1, i + 1, mid, :] if j < planes - 1 else halo[1, now, i, own, :]
            spread = (
                below + above
                + field[now, j, i, mid, :] + field[now, j, i + 2, mid, :]
                + field[now, j, i + 1, pl.ds(PAD - 1 + tile * PAD, PAD), :]
                + field[now, j, i + 1, pl.ds(PAD + 1 + tile * PAD, PAD), :]
                - 6.0 * here
            )
            later = 2.0 * here - field[other, j, i + 1, mid, :] + speed[j, i, own, :] * spread
            if step < STEPS - 1:
                field[other, j, i + 1, mid, :] = later
            else:
                far[j, i, own, :] = later

    def sums(which, tile):
        own = cells(0, tile)
        base = [far[j, 0, own, :] for j in which]

        def add(i, held):
            moved = [far[j, i, own, :] - b for j, b in zip(which, base)]
            return [(t + m, q + m * m) for (t, q), m in zip(held, moved)]

        zero = jnp.zeros((PAD, levels), jnp.float32)
        held = lax.fori_loop(0, lines, add, [(zero, zero) for _ in which], unroll=8)
        return [
            (b + t / lines, jnp.maximum(q - t * (t / lines), 0.0)) for b, (t, q) in zip(base, held)
        ]

    def send_stat(ref, slot):
        for n in range(1, blocks):
            pltpu.make_async_remote_copy(
                src_ref=ref, dst_ref=ref,
                send_sem=st_send.at[n, slot], recv_sem=st_recv.at[px, slot],
                device_id={"px": lax.rem(px + n, blocks)}, device_id_type=MESH,
            ).start()

    def edge_stat(tile, _):
        for n, (mean, squares) in enumerate(sums(edges, tile)):
            stat_edge[px, tile, 0, n] = mean
            stat_edge[px, tile, 1, n] = squares
        send_stat(stat_edge.at[px, tile], 1 + tile)
        return 0

    for step in range(STEPS):
        now, other = step % 2, (step + 1) % 2
        sides(step, "arrived")
        if step >= 1:
            sides(step - 1, "sent")

        which = range(planes)
        if step == STEPS - 1:
            which = edges
            if planes > 2:
                def middle(tile, _):
                    def row(i, _):
                        update(STEPS - 1, range(1, planes - 1), i, tile)
                        return 0

                    lax.fori_loop(0, lines, row, 0, unroll=4)
                    for n, (mean, squares) in enumerate(sums(range(1, planes - 1), tile)):
                        stat_in[px, 0, n, cells(0, tile), :] = mean
                        stat_in[px, 1, n, cells(0, tile), :] = squares
                    return 0

                lax.fori_loop(0, tiles, middle, 0)
                send_stat(stat_in.at[px], 0)

        def chunk(c, _, step=step, which=which):
            arrived_py(step, c)
            if step >= 1:
                sent_py(step - 1, c)
            tile, first_line = c // pieces, (c % pieces) * rows

            def row(r, _):
                update(step, which, first_line + r, tile)
                return 0

            lax.fori_loop(0, rows, row, 0, unroll=4)
            if step < STEPS - 1:
                forward_late(step + 1, c)
                send_py(step + 1, c)
            else:
                @pl.when(c % pieces == pieces - 1)
                def _():
                    edge_stat(tile, 0)
            return 0

        lax.fori_loop(0, chunks, chunk, 0)
        if step < STEPS - 1:
            sides(step + 1, "send")

    def settle(c, _):
        sent_py(STEPS - 1, c)
        return 0

    lax.fori_loop(0, chunks, settle, 0)
    sides(STEPS - 1, "sent")
    for slot, (_, _, via) in enumerate(jobs):
        @pl.when(py == via)
        def _(slot=slot):
            for step in range(STEPS):
                for c in range(chunks // 2):
                    done(relay.at[job_slot(slot), step, c], r_send.at[job_slot(slot), step, c])

    def combine(parts):
        mean = parts[0][0]
        for m, _ in parts[1:]:
            mean = mean + m
        mean = mean / blocks
        squares = jnp.zeros_like(mean)
        for m, q in parts:
            off = m - mean
            squares = squares + (q + lines * (off * off))
        return mean, lax.rsqrt(squares / (lines * blocks) + 0.0001)

    def gathered(at, slot):
        for n in range(1, blocks):
            source = lax.rem(px + n, blocks)
            done(at(px), st_send.at[n, slot])
            done(at(source), st_recv.at[source, slot])

    if planes > 2:
        gathered(lambda p: stat_in.at[p], 0)
        for n in range(planes - 2):
            mean_out[1 + n], scale_out[1 + n] = combine([(stat_in[p, 0, n], stat_in[p, 1, n]) for p in range(blocks)])
    for tile in range(tiles):
        gathered(lambda p: stat_edge.at[p, tile], 1 + tile)
        for n, j in enumerate(edges):
            own = pl.ds(tile * PAD, PAD)
            mean_out[j, own, :], scale_out[j, own, :] = combine(
                [(stat_edge[p, tile, 0, n], stat_edge[p, tile, 1, n]) for p in range(blocks)]
            )


def write_kernel(far, mean, scale, anomaly_out, far_out, scaled, sems):
    planes, lines = far.shape[:2]
    halves = sems.shape[2]
    rows = lines // halves
    whole = [(j, pl.ds(h * rows, rows), h) for j in range(planes) for h in range(halves)]
    keep = [pltpu.make_async_copy(far.at[j, at], far_out.at[j, at], sems.at[0, j, h]) for j, at, h in whole]
    copies = [pltpu.make_async_copy(scaled.at[j, at], anomaly_out.at[j, at], sems.at[1, j, h]) for j, at, h in whole]
    for copy in keep:
        copy.start()
    for (j, at, h), copy in zip(whole, copies):
        middle, factor = mean[j], scale[j]

        def row(i, _, j=j, h=h, middle=middle, factor=factor):
            scaled[j, h * rows + i] = (far[j, h * rows + i] - middle) * factor
            return 0

        lax.fori_loop(0, rows, row, 0, unroll=8)
        copy.start()
    for copy in keep + copies:
        copy.wait()


def shards(jobs, axes, field_now, earlier, speed_square):
    planes, lines, depth, levels = shape = field_now.shape
    tiles = depth // PAD
    pieces = 1
    chunks = tiles * pieces
    rows = lines // pieces
    held = max([1] + [[v for _, _, v in jobs].count(via) for _, _, via in jobs])
    blocks = axes["px"]
    dma = pltpu.SemaphoreType.DMA
    f32 = jnp.float32
    middle = max(planes - 2, 1)
    edges = min(planes, 2)
    vmem = pl.BlockSpec(memory_space=pltpu.VMEM)
    anywhere = pl.BlockSpec(memory_space=pl.ANY)
    far, mean, scale = pl.pallas_call(
        functools.partial(steps_kernel, jobs, pieces, axes),
        out_shape=[
            pltpu.VMEM(shape, f32),
            pltpu.VMEM((planes, depth, levels), f32),
            pltpu.VMEM((planes, depth, levels), f32),
        ],
        in_specs=[anywhere] * 3,
        out_specs=[vmem] * 3,
        scratch_shapes=[
            pltpu.VMEM((2, planes, lines + 2, depth + 2 * PAD, levels), f32),
            pltpu.VMEM(shape, f32),
            pltpu.VMEM((2, 2, lines, depth, levels), f32),
            pltpu.VMEM((held, STEPS, chunks // 2, rows, PAD, levels) if jobs else (1, 1, 1, 1, PAD, levels), f32),
            pltpu.VMEM((blocks, 2, middle, depth, levels), f32),
            pltpu.VMEM((blocks, tiles, 2, edges, PAD, levels), f32),
            dma((3,)),
            dma((2, 2, chunks)),
            dma((2, 2, chunks)),
            dma((held, STEPS, chunks // 2)),
            dma((held, STEPS, chunks // 2)),
            dma((2, 2, 2)),
            dma((2, 2, 2)),
            dma((blocks, 1 + tiles)),
            dma((blocks, 1 + tiles)),
        ],
        compiler_params=pltpu.CompilerParams(
            collective_id=0, has_side_effects=True, vmem_limit_bytes=LIMIT,
        ),
    )(field_now, earlier, speed_square)
    anomaly, far = pl.pallas_call(
        write_kernel,
        out_shape=[jax.ShapeDtypeStruct(shape, f32)] * 2,
        in_specs=[vmem] * 3,
        out_specs=[anywhere] * 2,
        scratch_shapes=[pltpu.VMEM(shape, f32), dma((2, planes, 2))],
        compiler_params=pltpu.CompilerParams(vmem_limit_bytes=24 * 2**20),
    )(far, mean, scale)
    return (anomaly, far)


def solution(mesh):
    axes = dict(mesh.shape)
    return jax.shard_map(
        functools.partial(shards, relays(mesh), axes),
        mesh=mesh,
        in_specs=(P("py", "px", "pz", None),) * 3,
        out_specs=(P("py", "px", "pz", None),) * 2,
        check_vma=False,
    )
```

```python
import functools

import jax
import jax.numpy as jnp
from jax import lax
from jax.experimental import pallas as pl
from jax.experimental.pallas import tpu as pltpu
from jax.sharding import PartitionSpec as P

STEPS = 4
PAD = 8
LENT = 5
LIMIT = 54 * 2**20
MESH = pl.DeviceIdType.MESH


def relays(mesh):
    devices = mesh.devices
    line = [devices[(n,) + (0,) * (devices.ndim - 1)] for n in range(devices.shape[0])]
    places = [getattr(device, "coords", None) for device in line]
    if any(place is None for place in places):
        return ()
    places = [tuple(place) for place in places]
    jobs = []
    for low in range(len(line) - 1):
        for a, b in ((low, low + 1), (low + 1, low)):
            turn = (places[a][0],) + places[b][1:]
            if turn in places and turn not in (places[a], places[b]):
                jobs.append((a, b, places.index(turn)))
    return tuple(jobs)


def paired(mesh):
    row = mesh.devices[(0,) * (mesh.devices.ndim - 1)]
    places = [(getattr(device, "coords", None), getattr(device, "core_on_chip", None)) for device in row]
    if len(places) % 2 or any(None in place for place in places):
        return False
    twos = [(places[n], places[n + 1]) for n in range(0, len(places), 2)]
    return all(tuple(a[0]) == tuple(b[0]) and (a[1], b[1]) == (0, 1) for a, b in twos)


def steps_kernel(jobs, pieces, lent, axes, f_ref, e_ref, c_ref, far, mean_out, scale_out,
                 field, speed, halo, relay, lent_in, stat_in, stat_edge, load_sem, py_send, py_recv,
                 r_send, r_recv, lent_send, lent_recv, side_send, side_recv, st_send, st_recv):
    planes, lines, depth, levels = c_ref.shape
    tiles = depth // PAD
    chunks = tiles * pieces
    rows = lines // pieces
    edges = sorted({0, planes - 1})
    inner = pl.ds(PAD, depth)
    me = {name: lax.axis_index(name) for name in axes}
    count = {name: axes[name] for name in axes}
    py = me["py"]

    staged = [
        pltpu.make_async_copy(f_ref.at[j, :, pl.ds(0, PAD)], far.at[j, :, pl.ds(0, PAD)], load_sem.at[3 + n])
        for n, j in enumerate(edges)
    ]
    for load in staged:
        load.start()

    barrier = pltpu.get_barrier_semaphore()
    greeted = 0
    met = sorted({(n, n + 1) for n in range(count["py"] - 1)} | {
        tuple(sorted(pair)) for a, b, via in jobs for pair in ((a, via), (via, b))
    })
    for low, high in met:
        for here, beyond in ((low, high), (high, low)):
            @pl.when(py == here)
            def _(beyond=beyond):
                pl.semaphore_signal(barrier, inc=1, device_id={"py": beyond}, device_id_type=MESH)
    known = sum((py == here).astype(jnp.int32) for pair in met for here in pair)
    for name in axes:
        if name == "py":
            continue
        for n in range(1, count[name]):
            pl.semaphore_signal(
                barrier, inc=1, device_id={name: lax.rem(me[name] + n, count[name])},
                device_id_type=MESH,
            )
            greeted += 1
    pl.semaphore_wait(barrier, known + greeted)

    def there(name, way):
        return me[name] < count[name] - 1 if way else me[name] > 0

    def done(ref, sem):
        pltpu.make_async_copy(ref, ref, sem).wait()

    def part(c, line, cell, held=(0, rows)):
        start = cell + (c // pieces) * PAD
        if cell % PAD == 0:
            start = pl.multiple_of(start, PAD)
        return pl.ds(line + (c % pieces) * rows + held[0], held[1]), pl.ds(start, PAD)

    def edge(step, c, way, held=(0, rows)):
        plane = planes - 1 if way else 0
        if step == 0:
            start = far if isinstance(c, int) else f_ref
            return start.at[(plane,) + part(c, 0, 0, held)]
        return field.at[(step % 2, plane) + part(c, 1, PAD, held)]

    def landing(step, c, side, held=(0, rows)):
        return halo.at[(side, step % 2) + part(c, 0, 0, held)]

    last = STEPS - 1
    own_part, lent_part = (0, rows - lent), (rows - lent, lent)
    mate = me["pz"] + 1 - 2 * lax.rem(me["pz"], 2)
    inner_core = lax.rem(me["pz"], 2) == 0

    def shares(way):
        busy = there("py", way)
        for a, b, _ in jobs:
            if b - a != 2 * way - 1:
                busy = jnp.logical_and(busy, py != a)
        return busy

    def pass_lent(c):
        if lent:
            for way in (0, 1):
                @pl.when(jnp.logical_and(jnp.logical_and(c == 2, jnp.logical_not(inner_core)), shares(way)))
                def _(way=way):
                    done(lent_in.at[way], lent_recv.at[way])
                    pltpu.make_async_remote_copy(
                        src_ref=lent_in.at[way],
                        dst_ref=landing(last, 1, 1 - way, lent_part),
                        send_sem=lent_send.at[way],
                        recv_sem=py_recv.at[1 - way, last % 2, 1],
                        device_id={"py": py + (2 * way - 1), "pz": mate}, device_id_type=MESH,
                    ).start()

    def send_py(step, c):
        for way in (0, 1):
            beyond = py + (2 * way - 1)
            direct = there("py", way)
            for slot, (a, b, via) in enumerate(jobs):
                if b - a != 2 * way - 1:
                    continue
                turned = jnp.logical_and(py == a, jnp.int32(c) % 2 == 0)
                direct = jnp.logical_and(direct, jnp.logical_not(turned))

                @pl.when(turned)
                def _(slot=slot, via=via, way=way):
                    pltpu.make_async_remote_copy(
                        src_ref=edge(step, c, way),
                        dst_ref=relay.at[job_slot(slot), step, c // 2],
                        send_sem=py_send.at[way, step % 2, c],
                        recv_sem=r_recv.at[job_slot(slot), step, c // 2],
                        device_id={"py": via}, device_id_type=MESH,
                    ).start()

            if lent and step == last:
                split = jnp.logical_and(jnp.logical_and(c == 1, inner_core), jnp.logical_and(direct, shares(way)))
                direct = jnp.logical_and(direct, jnp.logical_not(split))

                @pl.when(split)
                def _(way=way, beyond=beyond):
                    pltpu.make_async_remote_copy(
                        src_ref=edge(step, c, way, lent_part),
                        dst_ref=lent_in.at[way],
                        send_sem=py_send.at[way, step % 2, c],
                        recv_sem=lent_recv.at[way],
                        device_id={"pz": mate}, device_id_type=MESH,
                    ).start()
                    pltpu.make_async_remote_copy(
                        src_ref=edge(step, c, way, own_part),
                        dst_ref=landing(step, c, 1 - way, own_part),
                        send_sem=py_send.at[way, step % 2, c],
                        recv_sem=py_recv.at[1 - way, step % 2, c],
                        device_id={"py": beyond}, device_id_type=MESH,
                    ).start()

            @pl.when(direct)
            def _(way=way, beyond=beyond):
                pltpu.make_async_remote_copy(
                    src_ref=edge(step, c, way),
                    dst_ref=landing(step, c, 1 - way),
                    send_sem=py_send.at[way, step % 2, c],
                    recv_sem=py_recv.at[1 - way, step % 2, c],
                    device_id={"py": beyond}, device_id_type=MESH,
                ).start()

    def job_slot(slot):
        return [via for _, _, via in jobs[:slot]].count(jobs[slot][2])

    def forward(step, c):
        for slot, (a, b, via) in enumerate(jobs):
            @pl.when(py == via)
            def _(slot=slot, a=a, b=b):
                way = 1 if b > a else 0
                held = relay.at[job_slot(slot), step, c // 2]
                done(held, r_recv.at[job_slot(slot), step, c // 2])
                pltpu.make_async_remote_copy(
                    src_ref=held,
                    dst_ref=landing(step, c, 1 - way),
                    send_sem=r_send.at[job_slot(slot), step, c // 2],
                    recv_sem=py_recv.at[1 - way, step % 2, c],
                    device_id={"py": b}, device_id_type=MESH,
                ).start()

    def forward_late(step, c):
        if jobs and not isinstance(c, int):
            @pl.when(c % 2 == 1)
            def _():
                forward(step, c - 1)

    def sent_py(step, c):
        for way in (0, 1):
            @pl.when(there("py", way))
            def _(way=way):
                done(edge(step, c, way), py_send.at[way, step % 2, c])

    def arrived_py(step, c):
        for side in (0, 1):
            @pl.when(there("py", side))
            def _(side=side):
                done(landing(step, c, side), py_recv.at[side, step % 2, c])

    def side_source(step, name, way):
        if name == "px":
            at = lines - 1 if way else 0
            if step == 0:
                return f_ref.at[:, pl.ds(at, 1)]
            return field.at[step % 2, :, pl.ds(1 + at, 1), inner]
        at = depth - PAD if way else 0
        if step == 0:
            return f_ref.at[:, :, pl.ds(at, PAD)]
        return field.at[step % 2, :, pl.ds(1, lines), pl.ds(PAD + at, PAD)]

    def side_landing(slot, name, side):
        if name == "px":
            return field.at[slot, :, pl.ds(lines + 1 if side else 0, 1), inner]
        return field.at[slot, :, pl.ds(1, lines), pl.ds(PAD + depth if side else 0, PAD)]

    def sides(step, what):
        for n, name in enumerate(("px", "pz")):
            for way in (0, 1):
                @pl.when(there(name, way))
                def _(n=n, name=name, way=way):
                    if what == "send":
                        pltpu.make_async_remote_copy(
                            src_ref=side_source(step, name, way),
                            dst_ref=side_landing(step % 2, name, 1 - way),
                            send_sem=side_send.at[n, way, step % 2],
                            recv_sem=side_recv.at[n, 1 - way, step % 2],
                            device_id={name: me[name] + (2 * way - 1)}, device_id_type=MESH,
                        ).start()
                    elif what == "sent":
                        done(side_source(step, name, way), side_send.at[n, way, step % 2])
                    else:
                        done(side_landing(step % 2, name, way), side_recv.at[n, way, step % 2])

    whole = lambda slot: field.at[slot, :, pl.ds(1, lines), inner]
    loads = [
        pltpu.make_async_copy(f_ref, whole(0), load_sem.at[0]),
        pltpu.make_async_copy(e_ref, whole(1), load_sem.at[1]),
        pltpu.make_async_copy(c_ref, speed, load_sem.at[2]),
    ]

    def first(c, _):
        send_py(0, c)
        forward_late(0, c)
        return 0

    for load in staged:
        load.wait()
    first(0, 0)
    first(jnp.int32(1), 0)
    sides(0, "send")
    for load in loads:
        load.start()
    lax.fori_loop(2, chunks, first, 0)

    for way in (0, 1):
        @pl.when(jnp.logical_not(there("py", way)))
        def _(way=way):
            def clear(i, _):
                for slot in (0, 1):
                    halo[way, slot, i] = jnp.zeros((depth, levels), jnp.float32)
                return 0
            lax.fori_loop(0, lines, clear, 0)

        @pl.when(jnp.logical_not(there("px", way)))
        def _(way=way):
            for slot in (0, 1):
                for j in range(planes):
                    field[slot, j, lines + 1 if way else 0, inner, :] = jnp.zeros((depth, levels), jnp.float32)

        @pl.when(jnp.logical_not(there("pz", way)))
        def _(way=way):
            def clear(i, _):
                for slot in (0, 1):
                    for j in range(planes):
                        field[slot, j, 1 + i, pl.ds(PAD + depth if way else 0, PAD), :] = jnp.zeros((PAD, levels), jnp.float32)
                return 0
            lax.fori_loop(0, lines, clear, 0)

    for load in loads:
        load.wait()

    px, blocks = me["px"], count["px"]

    def cells(start, tile):
        start = start + tile * PAD
        return pl.ds(pl.multiple_of(start, PAD) if isinstance(start, jax.Array) and start.ndim == 0 else start, PAD)

    def update(step, which, i, tile):
        now, other = step % 2, (step + 1) % 2
        mid, own = cells(PAD, tile), cells(0, tile)
        for j in which:
            here = field[now, j, i + 1, mid, :]
            below = field[now, j - 1, i + 1, mid, :] if j else halo[0, now, i, own, :]
            above = field[now, j + 1, i + 1, mid, :] if j < planes - 1 else halo[1, now, i, own, :]
            spread = (
                below + above
                + field[now, j, i, mid, :] + field[now, j, i + 2, mid, :]
                + field[now, j, i + 1, pl.ds(PAD - 1 + tile * PAD, PAD), :]
                + field[now, j, i + 1, pl.ds(PAD + 1 + tile * PAD, PAD), :]
                - 6.0 * here
            )
            later = 2.0 * here - field[other, j, i + 1, mid, :] + speed[j, i, own, :] * spread
            if step < STEPS - 1:
                field[other, j, i + 1, mid, :] = later
            else:
                far[j, i, own, :] = later

    def sums(which, tile):
        own = cells(0, tile)
        base = [far[j, 0, own, :] for j in which]

        def add(i, held):
            moved = [far[j, i, own, :] - b for j, b in zip(which, base)]
            return [(t + m, q + m * m) for (t, q), m in zip(held, moved)]

        zero = jnp.zeros((PAD, levels), jnp.float32)
        held = lax.fori_loop(0, lines, add, [(zero, zero) for _ in which], unroll=8)
        return [
            (b + t / lines, jnp.maximum(q - t * (t / lines), 0.0)) for b, (t, q) in zip(base, held)
        ]

    def send_stat(ref, slot):
        for n in range(blocks - 1, 0, -1):
            for way in (0, 1):
                to = px + n if way else px - n

                @pl.when(to < blocks if way else to >= 0)
                def _(n=n, way=way, to=to):
                    pltpu.make_async_remote_copy(
                        src_ref=ref, dst_ref=ref,
                        send_sem=st_send.at[n if way else blocks - n, slot], recv_sem=st_recv.at[px, slot],
                        device_id={"px": to}, device_id_type=MESH,
                    ).start()

    def edge_stat(tile, _):
        for n, (mean, squares) in enumerate(sums(edges, tile)):
            stat_edge[px, tile, 0, n] = mean
            stat_edge[px, tile, 1, n] = squares
        send_stat(stat_edge.at[px, tile], 1 + tile)
        return 0

    for step in range(STEPS):
        now, other = step % 2, (step + 1) % 2
        sides(step, "arrived")
        if step >= 1:
            sides(step - 1, "sent")

        which = range(planes)
        if step == STEPS - 1:
            which = edges
            if planes > 2:
                def middle(tile, _):
                    def row(i, _):
                        update(STEPS - 1, range(1, planes - 1), i, tile)
                        return 0

                    lax.fori_loop(0, lines, row, 0, unroll=4)
                    for n, (mean, squares) in enumerate(sums(range(1, planes - 1), tile)):
                        stat_in[px, 0, n, cells(0, tile), :] = mean
                        stat_in[px, 1, n, cells(0, tile), :] = squares
                    return 0

                lax.fori_loop(0, tiles, middle, 0)
                send_stat(stat_in.at[px], 0)

        def chunk(c, _, step=step, which=which):
            arrived_py(step, c)
            if step >= 1:
                sent_py(step - 1, c)
            tile, first_line = c // pieces, (c % pieces) * rows

            def row(r, _):
                update(step, which, first_line + r, tile)
                return 0

            lax.fori_loop(0, rows, row, 0, unroll=4)
            if step < STEPS - 1:
                forward_late(step + 1, c)
                send_py(step + 1, c)
                if step + 1 == last:
                    pass_lent(c)
            else:
                @pl.when(c % pieces == pieces - 1)
                def _():
                    edge_stat(tile, 0)
            return 0

        lax.fori_loop(0, chunks, chunk, 0)
        if step < STEPS - 1:
            sides(step + 1, "send")

    def settle(c, _):
        sent_py(STEPS - 1, c)
        return 0

    lax.fori_loop(0, chunks, settle, 0)
    sides(STEPS - 1, "sent")
    for slot, (_, _, via) in enumerate(jobs):
        @pl.when(py == via)
        def _(slot=slot):
            for step in range(STEPS):
                for c in range(chunks // 2):
                    done(relay.at[job_slot(slot), step, c], r_send.at[job_slot(slot), step, c])

    if lent:
        for way in (0, 1):
            @pl.when(jnp.logical_and(jnp.logical_not(inner_core), shares(way)))
            def _(way=way):
                done(lent_in.at[way], lent_send.at[way])

    def combine(parts):
        mean = parts[0][0]
        for m, _ in parts[1:]:
            mean = mean + m
        mean = mean / blocks
        squares = jnp.zeros_like(mean)
        for m, q in parts:
            off = m - mean
            squares = squares + (q + lines * (off * off))
        return mean, lax.rsqrt(squares / (lines * blocks) + 0.0001)

    def gathered(at, slot):
        for n in range(1, blocks):
            source = lax.rem(px + n, blocks)
            done(at(px), st_send.at[n, slot])
            done(at(source), st_recv.at[source, slot])

    if planes > 2:
        gathered(lambda p: stat_in.at[p], 0)
        for n in range(planes - 2):
            mean_out[1 + n], scale_out[1 + n] = combine([(stat_in[p, 0, n], stat_in[p, 1, n]) for p in range(blocks)])
    for tile in range(tiles):
        gathered(lambda p: stat_edge.at[p, tile], 1 + tile)
        for n, j in enumerate(edges):
            own = pl.ds(tile * PAD, PAD)
            mean_out[j, own, :], scale_out[j, own, :] = combine(
                [(stat_edge[p, tile, 0, n], stat_edge[p, tile, 1, n]) for p in range(blocks)]
            )


def write_kernel(far, mean, scale, anomaly_out, far_out, scaled, sems):
    planes, lines = far.shape[:2]
    halves = sems.shape[2]
    rows = lines // halves
    whole = [(j, pl.ds(h * rows, rows), h) for j in range(planes) for h in range(halves)]
    keep = [pltpu.make_async_copy(far.at[j, at], far_out.at[j, at], sems.at[0, j, h]) for j, at, h in whole]
    copies = [pltpu.make_async_copy(scaled.at[j, at], anomaly_out.at[j, at], sems.at[1, j, h]) for j, at, h in whole]
    for copy in keep:
        copy.start()
    for (j, at, h), copy in zip(whole, copies):
        middle, factor = mean[j], scale[j]

        def row(i, _, j=j, h=h, middle=middle, factor=factor):
            scaled[j, h * rows + i] = (far[j, h * rows + i] - middle) * factor
            return 0

        lax.fori_loop(0, rows, row, 0, unroll=8)
        copy.start()
    for copy in keep + copies:
        copy.wait()


def shards(jobs, pairs, axes, field_now, earlier, speed_square):
    planes, lines, depth, levels = shape = field_now.shape
    tiles = depth // PAD
    pieces = 1
    chunks = tiles * pieces
    rows = lines // pieces
    lent = rows // LENT if pairs and pieces == 1 and chunks >= 4 else 0
    held = max([1] + [[v for _, _, v in jobs].count(via) for _, _, via in jobs])
    blocks = axes["px"]
    dma = pltpu.SemaphoreType.DMA
    f32 = jnp.float32
    middle = max(planes - 2, 1)
    edges = min(planes, 2)
    vmem = pl.BlockSpec(memory_space=pltpu.VMEM)
    anywhere = pl.BlockSpec(memory_space=pl.ANY)
    far, mean, scale = pl.pallas_call(
        functools.partial(steps_kernel, jobs, pieces, lent, axes),
        out_shape=[
            pltpu.VMEM(shape, f32),
            pltpu.VMEM((planes, depth, levels), f32),
            pltpu.VMEM((planes, depth, levels), f32),
        ],
        in_specs=[anywhere] * 3,
        out_specs=[vmem] * 3,
        scratch_shapes=[
            pltpu.VMEM((2, planes, lines + 2, depth + 2 * PAD, levels), f32),
            pltpu.VMEM(shape, f32),
            pltpu.VMEM((2, 2, lines, depth, levels), f32),
            pltpu.VMEM((held, STEPS, chunks // 2, rows, PAD, levels) if jobs else (1, 1, 1, 1, PAD, levels), f32),
            pltpu.VMEM((2, max(lent, 1), PAD, levels), f32),
            pltpu.VMEM((blocks, 2, middle, depth, levels), f32),
            pltpu.VMEM((blocks, tiles, 2, edges, PAD, levels), f32),
            dma((5,)),
            dma((2, 2, chunks)),
            dma((2, 2, chunks)),
            dma((held, STEPS, chunks // 2)),
            dma((held, STEPS, chunks // 2)),
            dma((2,)),
            dma((2,)),
            dma((2, 2, 2)),
            dma((2, 2, 2)),
            dma((blocks, 1 + tiles)),
            dma((blocks, 1 + tiles)),
        ],
        compiler_params=pltpu.CompilerParams(
            collective_id=0, has_side_effects=True, vmem_limit_bytes=LIMIT,
        ),
    )(field_now, earlier, speed_square)
    anomaly, far = pl.pallas_call(
        write_kernel,
        out_shape=[jax.ShapeDtypeStruct(shape, f32)] * 2,
        in_specs=[vmem] * 3,
        out_specs=[anywhere] * 2,
        scratch_shapes=[pltpu.VMEM(shape, f32), dma((2, planes, 2))],
        compiler_params=pltpu.CompilerParams(vmem_limit_bytes=24 * 2**20),
    )(far, mean, scale)
    return (anomaly, far)


def solution(mesh):
    axes = dict(mesh.shape)
    return jax.shard_map(
        functools.partial(shards, relays(mesh), paired(mesh), axes),
        mesh=mesh,
        in_specs=(P("py", "px", "pz", None),) * 3,
        out_specs=(P("py", "px", "pz", None),) * 2,
        check_vma=False,
    )
```

```python
import functools

import jax
import jax.numpy as jnp
from jax import lax
from jax.experimental import pallas as pl
from jax.experimental.pallas import tpu as pltpu
from jax.sharding import PartitionSpec as P

STEPS = 4
PAD = 8
LENT = 4
LIMIT = 54 * 2**20
MESH = pl.DeviceIdType.MESH


def relays(mesh):
    devices = mesh.devices
    line = [devices[(n,) + (0,) * (devices.ndim - 1)] for n in range(devices.shape[0])]
    places = [getattr(device, "coords", None) for device in line]
    if any(place is None for place in places):
        return ()
    places = [tuple(place) for place in places]
    jobs = []
    for low in range(len(line) - 1):
        for a, b in ((low, low + 1), (low + 1, low)):
            turn = (places[a][0],) + places[b][1:]
            if turn in places and turn not in (places[a], places[b]):
                jobs.append((a, b, places.index(turn)))
    return tuple(jobs)


def paired(mesh):
    row = mesh.devices[(0,) * (mesh.devices.ndim - 1)]
    places = [(getattr(device, "coords", None), getattr(device, "core_on_chip", None)) for device in row]
    if len(places) % 2 or any(None in place for place in places):
        return False
    twos = [(places[n], places[n + 1]) for n in range(0, len(places), 2)]
    return all(tuple(a[0]) == tuple(b[0]) and (a[1], b[1]) == (0, 1) for a, b in twos)


def steps_kernel(jobs, pieces, lent, axes, f_ref, e_ref, c_ref, far, mean_out, scale_out,
                 field, speed, halo, relay, lent_in, stat_in, stat_edge, load_sem, py_send, py_recv,
                 r_send, r_recv, lent_send, lent_recv, side_send, side_recv, st_send, st_recv):
    planes, lines, depth, levels = c_ref.shape
    tiles = depth // PAD
    chunks = tiles * pieces
    rows = lines // pieces
    edges = sorted({0, planes - 1})
    inner = pl.ds(PAD, depth)
    me = {name: lax.axis_index(name) for name in axes}
    count = {name: axes[name] for name in axes}
    py = me["py"]

    staged = [
        pltpu.make_async_copy(f_ref.at[j, :, pl.ds(0, PAD)], far.at[j, :, pl.ds(0, PAD)], load_sem.at[3 + n])
        for n, j in enumerate(edges)
    ]
    for load in staged:
        load.start()

    barrier = pltpu.get_barrier_semaphore()
    greeted = 0
    met = sorted({(n, n + 1) for n in range(count["py"] - 1)} | {
        tuple(sorted(pair)) for a, b, via in jobs for pair in ((a, via), (via, b))
    })
    for low, high in met:
        for here, beyond in ((low, high), (high, low)):
            @pl.when(py == here)
            def _(beyond=beyond):
                pl.semaphore_signal(barrier, inc=1, device_id={"py": beyond}, device_id_type=MESH)
    known = sum((py == here).astype(jnp.int32) for pair in met for here in pair)
    for name in axes:
        if name == "py":
            continue
        for n in range(1, count[name]):
            pl.semaphore_signal(
                barrier, inc=1, device_id={name: lax.rem(me[name] + n, count[name])},
                device_id_type=MESH,
            )
            greeted += 1
    pl.semaphore_wait(barrier, known + greeted)

    def there(name, way):
        return me[name] < count[name] - 1 if way else me[name] > 0

    def done(ref, sem):
        pltpu.make_async_copy(ref, ref, sem).wait()

    def part(c, line, cell, held=(0, rows)):
        start = cell + (c // pieces) * PAD
        if cell % PAD == 0:
            start = pl.multiple_of(start, PAD)
        return pl.ds(line + (c % pieces) * rows + held[0], held[1]), pl.ds(start, PAD)

    def edge(step, c, way, held=(0, rows)):
        plane = planes - 1 if way else 0
        if step == 0:
            start = far if isinstance(c, int) else f_ref
            return start.at[(plane,) + part(c, 0, 0, held)]
        return field.at[(step % 2, plane) + part(c, 1, PAD, held)]

    def landing(step, c, side, held=(0, rows)):
        return halo.at[(side, step % 2) + part(c, 0, 0, held)]

    last = STEPS - 1
    own_part, lent_part = (0, rows - lent), (rows - lent, lent)
    mate = me["pz"] + 1 - 2 * lax.rem(me["pz"], 2)
    inner_core = lax.rem(me["pz"], 2) == 0

    def shares(way):
        busy = there("py", way)
        for a, b, _ in jobs:
            if b - a != 2 * way - 1:
                busy = jnp.logical_and(busy, py != a)
        return busy

    def pass_lent(c):
        if lent:
            for way in (0, 1):
                @pl.when(jnp.logical_and(jnp.logical_and(c == 2, jnp.logical_not(inner_core)), shares(way)))
                def _(way=way):
                    done(lent_in.at[way], lent_recv.at[way])
                    pltpu.make_async_remote_copy(
                        src_ref=lent_in.at[way],
                        dst_ref=landing(last, 1, 1 - way, lent_part),
                        send_sem=lent_send.at[way],
                        recv_sem=py_recv.at[1 - way, last % 2, 1],
                        device_id={"py": py + (2 * way - 1), "pz": mate}, device_id_type=MESH,
                    ).start()

    def send_py(step, c):
        for way in (0, 1):
            beyond = py + (2 * way - 1)
            direct = there("py", way)
            for slot, (a, b, via) in enumerate(jobs):
                if b - a != 2 * way - 1:
                    continue
                turned = jnp.logical_and(py == a, jnp.int32(c) % 2 == 0)
                direct = jnp.logical_and(direct, jnp.logical_not(turned))

                @pl.when(turned)
                def _(slot=slot, via=via, way=way):
                    pltpu.make_async_remote_copy(
                        src_ref=edge(step, c, way),
                        dst_ref=relay.at[job_slot(slot), step, c // 2],
                        send_sem=py_send.at[way, step % 2, c],
                        recv_sem=r_recv.at[job_slot(slot), step, c // 2],
                        device_id={"py": via}, device_id_type=MESH,
                    ).start()

            if lent and step == last:
                split = jnp.logical_and(jnp.logical_and(c == 1, inner_core), jnp.logical_and(direct, shares(way)))
                direct = jnp.logical_and(direct, jnp.logical_not(split))

                @pl.when(split)
                def _(way=way, beyond=beyond):
                    pltpu.make_async_remote_copy(
                        src_ref=edge(step, c, way, lent_part),
                        dst_ref=lent_in.at[way],
                        send_sem=py_send.at[way, step % 2, c],
                        recv_sem=lent_recv.at[way],
                        device_id={"pz": mate}, device_id_type=MESH,
                    ).start()
                    pltpu.make_async_remote_copy(
                        src_ref=edge(step, c, way, own_part),
                        dst_ref=landing(step, c, 1 - way, own_part),
                        send_sem=py_send.at[way, step % 2, c],
                        recv_sem=py_recv.at[1 - way, step % 2, c],
                        device_id={"py": beyond}, device_id_type=MESH,
                    ).start()

            @pl.when(direct)
            def _(way=way, beyond=beyond):
                pltpu.make_async_remote_copy(
                    src_ref=edge(step, c, way),
                    dst_ref=landing(step, c, 1 - way),
                    send_sem=py_send.at[way, step % 2, c],
                    recv_sem=py_recv.at[1 - way, step % 2, c],
                    device_id={"py": beyond}, device_id_type=MESH,
                ).start()

    def job_slot(slot):
        return [via for _, _, via in jobs[:slot]].count(jobs[slot][2])

    def forward(step, c):
        for slot, (a, b, via) in enumerate(jobs):
            @pl.when(py == via)
            def _(slot=slot, a=a, b=b):
                way = 1 if b > a else 0
                held = relay.at[job_slot(slot), step, c // 2]
                done(held, r_recv.at[job_slot(slot), step, c // 2])
                pltpu.make_async_remote_copy(
                    src_ref=held,
                    dst_ref=landing(step, c, 1 - way),
                    send_sem=r_send.at[job_slot(slot), step, c // 2],
                    recv_sem=py_recv.at[1 - way, step % 2, c],
                    device_id={"py": b}, device_id_type=MESH,
                ).start()

    def forward_late(step, c):
        if jobs and not isinstance(c, int):
            @pl.when(c % 2 == 1)
            def _():
                forward(step, c - 1)

    def sent_py(step, c):
        for way in (0, 1):
            @pl.when(there("py", way))
            def _(way=way):
                done(edge(step, c, way), py_send.at[way, step % 2, c])

    def arrived_py(step, c):
        for side in (0, 1):
            @pl.when(there("py", side))
            def _(side=side):
                done(landing(step, c, side), py_recv.at[side, step % 2, c])

    def side_source(step, name, way):
        if name == "px":
            at = lines - 1 if way else 0
            if step == 0:
                return f_ref.at[:, pl.ds(at, 1)]
            return field.at[step % 2, :, pl.ds(1 + at, 1), inner]
        at = depth - PAD if way else 0
        if step == 0:
            return f_ref.at[:, :, pl.ds(at, PAD)]
        return field.at[step % 2, :, pl.ds(1, lines), pl.ds(PAD + at, PAD)]

    def side_landing(slot, name, side):
        if name == "px":
            return field.at[slot, :, pl.ds(lines + 1 if side else 0, 1), inner]
        return field.at[slot, :, pl.ds(1, lines), pl.ds(PAD + depth if side else 0, PAD)]

    def sides(step, what):
        for n, name in enumerate(("px", "pz")):
            for way in (0, 1):
                @pl.when(there(name, way))
                def _(n=n, name=name, way=way):
                    if what == "send":
                        pltpu.make_async_remote_copy(
                            src_ref=side_source(step, name, way),
                            dst_ref=side_landing(step % 2, name, 1 - way),
                            send_sem=side_send.at[n, way, step % 2],
                            recv_sem=side_recv.at[n, 1 - way, step % 2],
                            device_id={name: me[name] + (2 * way - 1)}, device_id_type=MESH,
                        ).start()
                    elif what == "sent":
                        done(side_source(step, name, way), side_send.at[n, way, step % 2])
                    else:
                        done(side_landing(step % 2, name, way), side_recv.at[n, way, step % 2])

    whole = lambda slot: field.at[slot, :, pl.ds(1, lines), inner]
    loads = [
        pltpu.make_async_copy(f_ref, whole(0), load_sem.at[0]),
        pltpu.make_async_copy(e_ref, whole(1), load_sem.at[1]),
        pltpu.make_async_copy(c_ref, speed, load_sem.at[2]),
    ]

    def first(c, _):
        send_py(0, c)
        forward_late(0, c)
        return 0

    for load in staged:
        load.wait()
    first(0, 0)
    first(jnp.int32(1), 0)
    sides(0, "send")
    for load in loads:
        load.start()
    lax.fori_loop(2, chunks, first, 0)

    for way in (0, 1):
        @pl.when(jnp.logical_not(there("py", way)))
        def _(way=way):
            def clear(i, _):
                for slot in (0, 1):
                    halo[way, slot, i] = jnp.zeros((depth, levels), jnp.float32)
                return 0
            lax.fori_loop(0, lines, clear, 0)

        @pl.when(jnp.logical_not(there("px", way)))
        def _(way=way):
            for slot in (0, 1):
                for j in range(planes):
                    field[slot, j, lines + 1 if way else 0, inner, :] = jnp.zeros((depth, levels), jnp.float32)

        @pl.when(jnp.logical_not(there("pz", way)))
        def _(way=way):
            def clear(i, _):
                for slot in (0, 1):
                    for j in range(planes):
                        field[slot, j, 1 + i, pl.ds(PAD + depth if way else 0, PAD), :] = jnp.zeros((PAD, levels), jnp.float32)
                return 0
            lax.fori_loop(0, lines, clear, 0)

    for load in loads:
        load.wait()

    px, blocks = me["px"], count["px"]

    def cells(start, tile):
        start = start + tile * PAD
        return pl.ds(pl.multiple_of(start, PAD) if isinstance(start, jax.Array) and start.ndim == 0 else start, PAD)

    def update(step, which, i, tile):
        now, other = step % 2, (step + 1) % 2
        mid, own = cells(PAD, tile), cells(0, tile)
        for j in which:
            here = field[now, j, i + 1, mid, :]
            below = field[now, j - 1, i + 1, mid, :] if j else halo[0, now, i, own, :]
            above = field[now, j + 1, i + 1, mid, :] if j < planes - 1 else halo[1, now, i, own, :]
            spread = (
                below + above
                + field[now, j, i, mid, :] + field[now, j, i + 2, mid, :]
                + field[now, j, i + 1, pl.ds(PAD - 1 + tile * PAD, PAD), :]
                + field[now, j, i + 1, pl.ds(PAD + 1 + tile * PAD, PAD), :]
                - 6.0 * here
            )
            later = 2.0 * here - field[other, j, i + 1, mid, :] + speed[j, i, own, :] * spread
            if step < STEPS - 1:
                field[other, j, i + 1, mid, :] = later
            else:
                far[j, i, own, :] = later

    def sums(which, tile):
        own = cells(0, tile)
        base = [far[j, 0, own, :] for j in which]

        def add(i, held):
            moved = [far[j, i, own, :] - b for j, b in zip(which, base)]
            return [(t + m, q + m * m) for (t, q), m in zip(held, moved)]

        zero = jnp.zeros((PAD, levels), jnp.float32)
        held = lax.fori_loop(0, lines, add, [(zero, zero) for _ in which], unroll=8)
        return [
            (b + t / lines, jnp.maximum(q - t * (t / lines), 0.0)) for b, (t, q) in zip(base, held)
        ]

    def send_stat(ref, slot):
        for n in range(blocks - 1, 0, -1):
            for way in (0, 1):
                to = px + n if way else px - n

                @pl.when(to < blocks if way else to >= 0)
                def _(n=n, way=way, to=to):
                    pltpu.make_async_remote_copy(
                        src_ref=ref, dst_ref=ref,
                        send_sem=st_send.at[n if way else blocks - n, slot], recv_sem=st_recv.at[px, slot],
                        device_id={"px": to}, device_id_type=MESH,
                    ).start()

    def edge_stat(tile, _):
        for n, (mean, squares) in enumerate(sums(edges, tile)):
            stat_edge[px, tile, 0, n] = mean
            stat_edge[px, tile, 1, n] = squares
        send_stat(stat_edge.at[px, tile], 1 + tile)
        return 0

    for step in range(STEPS):
        now, other = step % 2, (step + 1) % 2
        sides(step, "arrived")
        if step >= 1:
            sides(step - 1, "sent")

        which = range(planes)
        if step == STEPS - 1:
            which = edges
            if planes > 2:
                def middle(tile, _):
                    def row(i, _):
                        update(STEPS - 1, range(1, planes - 1), i, tile)
                        return 0

                    lax.fori_loop(0, lines, row, 0, unroll=4)
                    for n, (mean, squares) in enumerate(sums(range(1, planes - 1), tile)):
                        stat_in[px, 0, n, cells(0, tile), :] = mean
                        stat_in[px, 1, n, cells(0, tile), :] = squares
                    return 0

                lax.fori_loop(0, tiles, middle, 0)
                send_stat(stat_in.at[px], 0)

        def chunk(c, _, step=step, which=which):
            arrived_py(step, c)
            if step >= 1:
                sent_py(step - 1, c)
            tile, first_line = c // pieces, (c % pieces) * rows

            def row(r, _):
                update(step, which, first_line + r, tile)
                return 0

            lax.fori_loop(0, rows, row, 0, unroll=4)
            if step < STEPS - 1:
                forward_late(step + 1, c)
                send_py(step + 1, c)
                if step + 1 == last:
                    pass_lent(c)
            else:
                @pl.when(c % pieces == pieces - 1)
                def _():
                    edge_stat(tile, 0)
            return 0

        lax.fori_loop(0, chunks, chunk, 0)
        if step < STEPS - 1:
            sides(step + 1, "send")

    def settle(c, _):
        sent_py(STEPS - 1, c)
        return 0

    lax.fori_loop(0, chunks, settle, 0)
    sides(STEPS - 1, "sent")
    for slot, (_, _, via) in enumerate(jobs):
        @pl.when(py == via)
        def _(slot=slot):
            for step in range(STEPS):
                for c in range(chunks // 2):
                    done(relay.at[job_slot(slot), step, c], r_send.at[job_slot(slot), step, c])

    if lent:
        for way in (0, 1):
            @pl.when(jnp.logical_and(jnp.logical_not(inner_core), shares(way)))
            def _(way=way):
                done(lent_in.at[way], lent_send.at[way])

    def combine(parts):
        mean = parts[0][0]
        for m, _ in parts[1:]:
            mean = mean + m
        mean = mean / blocks
        squares = jnp.zeros_like(mean)
        for m, q in parts:
            off = m - mean
            squares = squares + (q + lines * (off * off))
        return mean, lax.rsqrt(squares / (lines * blocks) + 0.0001)

    def gathered(at, slot):
        for n in range(1, blocks):
            source = lax.rem(px + n, blocks)
            done(at(px), st_send.at[n, slot])
            done(at(source), st_recv.at[source, slot])

    if planes > 2:
        gathered(lambda p: stat_in.at[p], 0)
        for n in range(planes - 2):
            mean_out[1 + n], scale_out[1 + n] = combine([(stat_in[p, 0, n], stat_in[p, 1, n]) for p in range(blocks)])
    for tile in range(tiles):
        gathered(lambda p: stat_edge.at[p, tile], 1 + tile)
        for n, j in enumerate(edges):
            own = pl.ds(tile * PAD, PAD)
            mean_out[j, own, :], scale_out[j, own, :] = combine(
                [(stat_edge[p, tile, 0, n], stat_edge[p, tile, 1, n]) for p in range(blocks)]
            )


def write_kernel(far, mean, scale, anomaly_out, far_out, scaled, sems):
    planes, lines = far.shape[:2]
    halves = sems.shape[2]
    rows = lines // halves
    whole = [(j, pl.ds(h * rows, rows), h) for j in range(planes) for h in range(halves)]
    keep = [pltpu.make_async_copy(far.at[j, at], far_out.at[j, at], sems.at[0, j, h]) for j, at, h in whole]
    copies = [pltpu.make_async_copy(scaled.at[j, at], anomaly_out.at[j, at], sems.at[1, j, h]) for j, at, h in whole]
    for copy in keep:
        copy.start()
    for (j, at, h), copy in zip(whole, copies):
        middle, factor = mean[j], scale[j]

        def row(i, _, j=j, h=h, middle=middle, factor=factor):
            scaled[j, h * rows + i] = (far[j, h * rows + i] - middle) * factor
            return 0

        lax.fori_loop(0, rows, row, 0, unroll=8)
        copy.start()
    for copy in keep + copies:
        copy.wait()


def shards(jobs, pairs, axes, field_now, earlier, speed_square):
    planes, lines, depth, levels = shape = field_now.shape
    tiles = depth // PAD
    pieces = 1
    chunks = tiles * pieces
    rows = lines // pieces
    lent = rows // LENT if pairs and pieces == 1 and chunks >= 4 else 0
    held = max([1] + [[v for _, _, v in jobs].count(via) for _, _, via in jobs])
    blocks = axes["px"]
    dma = pltpu.SemaphoreType.DMA
    f32 = jnp.float32
    middle = max(planes - 2, 1)
    edges = min(planes, 2)
    vmem = pl.BlockSpec(memory_space=pltpu.VMEM)
    anywhere = pl.BlockSpec(memory_space=pl.ANY)
    far, mean, scale = pl.pallas_call(
        functools.partial(steps_kernel, jobs, pieces, lent, axes),
        out_shape=[
            pltpu.VMEM(shape, f32),
            pltpu.VMEM((planes, depth, levels), f32),
            pltpu.VMEM((planes, depth, levels), f32),
        ],
        in_specs=[anywhere] * 3,
        out_specs=[vmem] * 3,
        scratch_shapes=[
            pltpu.VMEM((2, planes, lines + 2, depth + 2 * PAD, levels), f32),
            pltpu.VMEM(shape, f32),
            pltpu.VMEM((2, 2, lines, depth, levels), f32),
            pltpu.VMEM((held, STEPS, chunks // 2, rows, PAD, levels) if jobs else (1, 1, 1, 1, PAD, levels), f32),
            pltpu.VMEM((2, max(lent, 1), PAD, levels), f32),
            pltpu.VMEM((blocks, 2, middle, depth, levels), f32),
            pltpu.VMEM((blocks, tiles, 2, edges, PAD, levels), f32),
            dma((5,)),
            dma((2, 2, chunks)),
            dma((2, 2, chunks)),
            dma((held, STEPS, chunks // 2)),
            dma((held, STEPS, chunks // 2)),
            dma((2,)),
            dma((2,)),
            dma((2, 2, 2)),
            dma((2, 2, 2)),
            dma((blocks, 1 + tiles)),
            dma((blocks, 1 + tiles)),
        ],
        compiler_params=pltpu.CompilerParams(
            collective_id=0, has_side_effects=True, vmem_limit_bytes=LIMIT,
        ),
    )(field_now, earlier, speed_square)
    anomaly, far = pl.pallas_call(
        write_kernel,
        out_shape=[jax.ShapeDtypeStruct(shape, f32)] * 2,
        in_specs=[vmem] * 3,
        out_specs=[anywhere] * 2,
        scratch_shapes=[pltpu.VMEM(shape, f32), dma((2, planes, 2))],
        compiler_params=pltpu.CompilerParams(vmem_limit_bytes=24 * 2**20),
    )(far, mean, scale)
    return (anomaly, far)


def solution(mesh):
    axes = dict(mesh.shape)
    return jax.shard_map(
        functools.partial(shards, relays(mesh), paired(mesh), axes),
        mesh=mesh,
        in_specs=(P("py", "px", "pz", None),) * 3,
        out_specs=(P("py", "px", "pz", None),) * 2,
        check_vma=False,
    )
```

```python
import functools

import jax
import jax.numpy as jnp
from jax import lax
from jax.experimental import pallas as pl
from jax.experimental.pallas import tpu as pltpu
from jax.sharding import PartitionSpec as P

STEPS = 4
PAD = 8
LENT = 4
END = 4
LIMIT = 54 * 2**20
MESH = pl.DeviceIdType.MESH


def relays(mesh):
    devices = mesh.devices
    line = [devices[(n,) + (0,) * (devices.ndim - 1)] for n in range(devices.shape[0])]
    places = [getattr(device, "coords", None) for device in line]
    if any(place is None for place in places):
        return ()
    places = [tuple(place) for place in places]
    jobs = []
    for low in range(len(line) - 1):
        for a, b in ((low, low + 1), (low + 1, low)):
            turn = (places[a][0],) + places[b][1:]
            if turn in places and turn not in (places[a], places[b]):
                jobs.append((a, b, places.index(turn)))
    return tuple(jobs)


def paired(mesh):
    row = mesh.devices[(0,) * (mesh.devices.ndim - 1)]
    places = [(getattr(device, "coords", None), getattr(device, "core_on_chip", None)) for device in row]
    if len(places) % 2 or any(None in place for place in places):
        return False
    twos = [(places[n], places[n + 1]) for n in range(0, len(places), 2)]
    return all(tuple(a[0]) == tuple(b[0]) and (a[1], b[1]) == (0, 1) for a, b in twos)


def steps_kernel(jobs, pieces, lent, end, axes, f_ref, e_ref, c_ref, far, mean_out, scale_out,
                 field, speed, halo, relay, lent_in, stat_in, stat_edge, load_sem, py_send, py_recv,
                 r_send, r_recv, lent_send, lent_recv, end_recv, side_send, side_recv, st_send, st_recv):
    planes, lines, depth, levels = c_ref.shape
    tiles = depth // PAD
    chunks = tiles * pieces
    rows = lines // pieces
    edges = sorted({0, planes - 1})
    inner = pl.ds(PAD, depth)
    me = {name: lax.axis_index(name) for name in axes}
    count = {name: axes[name] for name in axes}
    py = me["py"]

    staged = [
        pltpu.make_async_copy(f_ref.at[j, :, pl.ds(0, PAD)], far.at[j, :, pl.ds(0, PAD)], load_sem.at[3 + n])
        for n, j in enumerate(edges)
    ]
    for load in staged:
        load.start()

    barrier = pltpu.get_barrier_semaphore()
    greeted = 0
    met = sorted({(n, n + 1) for n in range(count["py"] - 1)} | {
        tuple(sorted(pair)) for a, b, via in jobs for pair in ((a, via), (via, b))
    })
    for low, high in met:
        for here, beyond in ((low, high), (high, low)):
            @pl.when(py == here)
            def _(beyond=beyond):
                pl.semaphore_signal(barrier, inc=1, device_id={"py": beyond}, device_id_type=MESH)
    known = sum((py == here).astype(jnp.int32) for pair in met for here in pair)
    for name in axes:
        if name == "py":
            continue
        for n in range(1, count[name]):
            pl.semaphore_signal(
                barrier, inc=1, device_id={name: lax.rem(me[name] + n, count[name])},
                device_id_type=MESH,
            )
            greeted += 1
    pl.semaphore_wait(barrier, known + greeted)

    def there(name, way):
        return me[name] < count[name] - 1 if way else me[name] > 0

    def done(ref, sem):
        pltpu.make_async_copy(ref, ref, sem).wait()

    def part(c, line, cell, held=(0, rows)):
        start = cell + (c // pieces) * PAD
        if cell % PAD == 0:
            start = pl.multiple_of(start, PAD)
        return pl.ds(line + (c % pieces) * rows + held[0], held[1]), pl.ds(start, PAD)

    def edge(step, c, way, held=(0, rows)):
        plane = planes - 1 if way else 0
        if step == 0:
            start = far if isinstance(c, int) else f_ref
            return start.at[(plane,) + part(c, 0, 0, held)]
        return field.at[(step % 2, plane) + part(c, 1, PAD, held)]

    def landing(step, c, side, held=(0, rows)):
        return halo.at[(side, step % 2) + part(c, 0, 0, held)]

    last = STEPS - 1
    own_part, lent_part = (0, rows - lent), (rows - lent, lent)
    head_part, end_part = (0, rows - end), (rows - end, end)
    mate = me["pz"] + 1 - 2 * lax.rem(me["pz"], 2)
    inner_core = lax.rem(me["pz"], 2) == 0

    def shares(way):
        busy = there("py", way)
        for a, b, _ in jobs:
            if b - a != 2 * way - 1:
                busy = jnp.logical_and(busy, py != a)
        return busy

    def pass_lent(c):
        if lent:
            for way in (0, 1):
                @pl.when(jnp.logical_and(jnp.logical_and(c == 2, jnp.logical_not(inner_core)), shares(way)))
                def _(way=way):
                    done(lent_in.at[way], lent_recv.at[way])
                    pltpu.make_async_remote_copy(
                        src_ref=lent_in.at[way],
                        dst_ref=landing(last, 1, 1 - way, lent_part),
                        send_sem=lent_send.at[way],
                        recv_sem=py_recv.at[1 - way, last % 2, 1],
                        device_id={"py": py + (2 * way - 1), "pz": mate}, device_id_type=MESH,
                    ).start()

    def send_py(step, c):
        for way in (0, 1):
            beyond = py + (2 * way - 1)
            direct = there("py", way)
            for slot, (a, b, via) in enumerate(jobs):
                if b - a != 2 * way - 1:
                    continue
                turned = jnp.logical_and(py == a, jnp.int32(c) % 2 == 0)
                direct = jnp.logical_and(direct, jnp.logical_not(turned))

                @pl.when(turned)
                def _(slot=slot, via=via, way=way):
                    pltpu.make_async_remote_copy(
                        src_ref=edge(step, c, way),
                        dst_ref=relay.at[job_slot(slot), step, c // 2],
                        send_sem=py_send.at[way, step % 2, c],
                        recv_sem=r_recv.at[job_slot(slot), step, c // 2],
                        device_id={"py": via}, device_id_type=MESH,
                    ).start()

            if lent and step == last:
                split = jnp.logical_and(jnp.logical_and(c == 1, inner_core), jnp.logical_and(direct, shares(way)))
                direct = jnp.logical_and(direct, jnp.logical_not(split))

                @pl.when(split)
                def _(way=way, beyond=beyond):
                    pltpu.make_async_remote_copy(
                        src_ref=edge(step, c, way, lent_part),
                        dst_ref=lent_in.at[way],
                        send_sem=py_send.at[way, step % 2, c],
                        recv_sem=lent_recv.at[way],
                        device_id={"pz": mate}, device_id_type=MESH,
                    ).start()
                    pltpu.make_async_remote_copy(
                        src_ref=edge(step, c, way, own_part),
                        dst_ref=landing(step, c, 1 - way, own_part),
                        send_sem=py_send.at[way, step % 2, c],
                        recv_sem=py_recv.at[1 - way, step % 2, c],
                        device_id={"py": beyond}, device_id_type=MESH,
                    ).start()

            if end and step == last:
                ends = jnp.logical_and(direct, c == chunks - 1)
                direct = jnp.logical_and(direct, c != chunks - 1)

                @pl.when(ends)
                def _(way=way, beyond=beyond):
                    for held, sem in ((head_part, py_recv.at[1 - way, step % 2, c]), (end_part, end_recv.at[1 - way])):
                        pltpu.make_async_remote_copy(
                            src_ref=edge(step, c, way, held),
                            dst_ref=landing(step, c, 1 - way, held),
                            send_sem=py_send.at[way, step % 2, c],
                            recv_sem=sem,
                            device_id={"py": beyond}, device_id_type=MESH,
                        ).start()

            @pl.when(direct)
            def _(way=way, beyond=beyond):
                pltpu.make_async_remote_copy(
                    src_ref=edge(step, c, way),
                    dst_ref=landing(step, c, 1 - way),
                    send_sem=py_send.at[way, step % 2, c],
                    recv_sem=py_recv.at[1 - way, step % 2, c],
                    device_id={"py": beyond}, device_id_type=MESH,
                ).start()

    def job_slot(slot):
        return [via for _, _, via in jobs[:slot]].count(jobs[slot][2])

    def forward(step, c):
        for slot, (a, b, via) in enumerate(jobs):
            @pl.when(py == via)
            def _(slot=slot, a=a, b=b):
                way = 1 if b > a else 0
                held = relay.at[job_slot(slot), step, c // 2]
                done(held, r_recv.at[job_slot(slot), step, c // 2])
                pltpu.make_async_remote_copy(
                    src_ref=held,
                    dst_ref=landing(step, c, 1 - way),
                    send_sem=r_send.at[job_slot(slot), step, c // 2],
                    recv_sem=py_recv.at[1 - way, step % 2, c],
                    device_id={"py": b}, device_id_type=MESH,
                ).start()

    def forward_late(step, c):
        if jobs and not isinstance(c, int):
            @pl.when(c % 2 == 1)
            def _():
                forward(step, c - 1)

    def sent_py(step, c):
        for way in (0, 1):
            @pl.when(there("py", way))
            def _(way=way):
                done(edge(step, c, way), py_send.at[way, step % 2, c])

    def arrived_py(step, c):
        for side in (0, 1):
            @pl.when(there("py", side))
            def _(side=side):
                done(landing(step, c, side), py_recv.at[side, step % 2, c])

    def side_source(step, name, way):
        if name == "px":
            at = lines - 1 if way else 0
            if step == 0:
                return f_ref.at[:, pl.ds(at, 1)]
            return field.at[step % 2, :, pl.ds(1 + at, 1), inner]
        at = depth - PAD if way else 0
        if step == 0:
            return f_ref.at[:, :, pl.ds(at, PAD)]
        return field.at[step % 2, :, pl.ds(1, lines), pl.ds(PAD + at, PAD)]

    def side_landing(slot, name, side):
        if name == "px":
            return field.at[slot, :, pl.ds(lines + 1 if side else 0, 1), inner]
        return field.at[slot, :, pl.ds(1, lines), pl.ds(PAD + depth if side else 0, PAD)]

    def sides(step, what):
        for n, name in enumerate(("px", "pz")):
            for way in (0, 1):
                @pl.when(there(name, way))
                def _(n=n, name=name, way=way):
                    if what == "send":
                        pltpu.make_async_remote_copy(
                            src_ref=side_source(step, name, way),
                            dst_ref=side_landing(step % 2, name, 1 - way),
                            send_sem=side_send.at[n, way, step % 2],
                            recv_sem=side_recv.at[n, 1 - way, step % 2],
                            device_id={name: me[name] + (2 * way - 1)}, device_id_type=MESH,
                        ).start()
                    elif what == "sent":
                        done(side_source(step, name, way), side_send.at[n, way, step % 2])
                    else:
                        done(side_landing(step % 2, name, way), side_recv.at[n, way, step % 2])

    whole = lambda slot: field.at[slot, :, pl.ds(1, lines), inner]
    loads = [
        pltpu.make_async_copy(f_ref, whole(0), load_sem.at[0]),
        pltpu.make_async_copy(e_ref, whole(1), load_sem.at[1]),
        pltpu.make_async_copy(c_ref, speed, load_sem.at[2]),
    ]

    def first(c, _):
        send_py(0, c)
        forward_late(0, c)
        return 0

    for load in staged:
        load.wait()
    first(0, 0)
    first(jnp.int32(1), 0)
    sides(0, "send")
    for load in loads:
        load.start()
    lax.fori_loop(2, chunks, first, 0)

    for way in (0, 1):
        @pl.when(jnp.logical_not(there("py", way)))
        def _(way=way):
            def clear(i, _):
                for slot in (0, 1):
                    halo[way, slot, i] = jnp.zeros((depth, levels), jnp.float32)
                return 0
            lax.fori_loop(0, lines, clear, 0)

        @pl.when(jnp.logical_not(there("px", way)))
        def _(way=way):
            for slot in (0, 1):
                for j in range(planes):
                    field[slot, j, lines + 1 if way else 0, inner, :] = jnp.zeros((depth, levels), jnp.float32)

        @pl.when(jnp.logical_not(there("pz", way)))
        def _(way=way):
            def clear(i, _):
                for slot in (0, 1):
                    for j in range(planes):
                        field[slot, j, 1 + i, pl.ds(PAD + depth if way else 0, PAD), :] = jnp.zeros((PAD, levels), jnp.float32)
                return 0
            lax.fori_loop(0, lines, clear, 0)

    for load in loads:
        load.wait()

    px, blocks = me["px"], count["px"]

    def cells(start, tile):
        start = start + tile * PAD
        return pl.ds(pl.multiple_of(start, PAD) if isinstance(start, jax.Array) and start.ndim == 0 else start, PAD)

    def update(step, which, i, tile):
        now, other = step % 2, (step + 1) % 2
        mid, own = cells(PAD, tile), cells(0, tile)
        for j in which:
            here = field[now, j, i + 1, mid, :]
            below = field[now, j - 1, i + 1, mid, :] if j else halo[0, now, i, own, :]
            above = field[now, j + 1, i + 1, mid, :] if j < planes - 1 else halo[1, now, i, own, :]
            spread = (
                below + above
                + field[now, j, i, mid, :] + field[now, j, i + 2, mid, :]
                + field[now, j, i + 1, pl.ds(PAD - 1 + tile * PAD, PAD), :]
                + field[now, j, i + 1, pl.ds(PAD + 1 + tile * PAD, PAD), :]
                - 6.0 * here
            )
            later = 2.0 * here - field[other, j, i + 1, mid, :] + speed[j, i, own, :] * spread
            if step < STEPS - 1:
                field[other, j, i + 1, mid, :] = later
            else:
                far[j, i, own, :] = later

    def sums(which, tile, held=None, first=0, stop=lines):
        own = cells(0, tile)
        base = [far[j, 0, own, :] for j in which]

        def add(i, held):
            moved = [far[j, i, own, :] - b for j, b in zip(which, base)]
            return [(t + m, q + m * m) for (t, q), m in zip(held, moved)]

        zero = jnp.zeros((PAD, levels), jnp.float32)
        held = [(zero, zero) for _ in which] if held is None else held
        held = lax.fori_loop(first, stop, add, held, unroll=8)
        return held if stop < lines else [
            (b + t / lines, jnp.maximum(q - t * (t / lines), 0.0)) for b, (t, q) in zip(base, held)
        ]

    def send_stat(ref, slot):
        for n in range(blocks - 1, 0, -1):
            for way in (0, 1):
                to = px + n if way else px - n

                @pl.when(to < blocks if way else to >= 0)
                def _(n=n, way=way, to=to):
                    pltpu.make_async_remote_copy(
                        src_ref=ref, dst_ref=ref,
                        send_sem=st_send.at[n if way else blocks - n, slot], recv_sem=st_recv.at[px, slot],
                        device_id={"px": to}, device_id_type=MESH,
                    ).start()

    def edge_stat(tile, found):
        for n, (mean, squares) in enumerate(found):
            stat_edge[px, tile, 0, n] = mean
            stat_edge[px, tile, 1, n] = squares
        send_stat(stat_edge.at[px, tile], 1 + tile)
        return 0

    for step in range(STEPS):
        now, other = step % 2, (step + 1) % 2
        sides(step, "arrived")
        if step >= 1:
            sides(step - 1, "sent")

        which = range(planes)
        if step == STEPS - 1:
            which = edges
            if planes > 2:
                def middle(tile, _):
                    def row(i, _):
                        update(STEPS - 1, range(1, planes - 1), i, tile)
                        return 0

                    lax.fori_loop(0, lines, row, 0, unroll=4)
                    for n, (mean, squares) in enumerate(sums(range(1, planes - 1), tile)):
                        stat_in[px, 0, n, cells(0, tile), :] = mean
                        stat_in[px, 1, n, cells(0, tile), :] = squares
                    return 0

                lax.fori_loop(0, tiles, middle, 0)
                send_stat(stat_in.at[px], 0)

        def chunk(c, _, step=step, which=which):
            arrived_py(step, c)
            if step >= 1:
                sent_py(step - 1, c)
            tile, first_line = c // pieces, (c % pieces) * rows

            def row(r, _):
                update(step, which, first_line + r, tile)
                return 0

            lax.fori_loop(0, rows, row, 0, unroll=4)
            if step < STEPS - 1:
                forward_late(step + 1, c)
                send_py(step + 1, c)
                if step + 1 == last:
                    pass_lent(c)
            else:
                @pl.when(c % pieces == pieces - 1)
                def _():
                    edge_stat(tile, sums(edges, tile))
            return 0

        lax.fori_loop(0, chunks - 1 if end and step == last else chunks, chunk, 0)
        if end and step == last:
            c, held = chunks - 1, None
            sent_py(step - 1, c)
            for first, n in (head_part, end_part):
                for side in (0, 1):
                    @pl.when(there("py", side))
                    def _(side=side, first=first, n=n):
                        arrival = py_recv.at[side, last % 2, c] if first == 0 else end_recv.at[side]
                        done(landing(last, c, side, (first, n)), arrival)

                def row(r, _):
                    update(step, edges, r, c)
                    return 0

                lax.fori_loop(first, first + n, row, 0, unroll=4)
                held = sums(edges, c, held, first, first + n)
            edge_stat(c, held)
        if step < STEPS - 1:
            sides(step + 1, "send")

    def settle(c, _):
        sent_py(STEPS - 1, c)
        return 0

    lax.fori_loop(0, chunks, settle, 0)
    sides(STEPS - 1, "sent")
    for slot, (_, _, via) in enumerate(jobs):
        @pl.when(py == via)
        def _(slot=slot):
            for step in range(STEPS):
                for c in range(chunks // 2):
                    done(relay.at[job_slot(slot), step, c], r_send.at[job_slot(slot), step, c])

    if lent:
        for way in (0, 1):
            @pl.when(jnp.logical_and(jnp.logical_not(inner_core), shares(way)))
            def _(way=way):
                done(lent_in.at[way], lent_send.at[way])

    def combine(parts):
        mean = parts[0][0]
        for m, _ in parts[1:]:
            mean = mean + m
        mean = mean / blocks
        squares = jnp.zeros_like(mean)
        for m, q in parts:
            off = m - mean
            squares = squares + (q + lines * (off * off))
        return mean, lax.rsqrt(squares / (lines * blocks) + 0.0001)

    def gathered(at, slot):
        for n in range(1, blocks):
            source = lax.rem(px + n, blocks)
            done(at(px), st_send.at[n, slot])
            done(at(source), st_recv.at[source, slot])

    if planes > 2:
        gathered(lambda p: stat_in.at[p], 0)
        for n in range(planes - 2):
            mean_out[1 + n], scale_out[1 + n] = combine([(stat_in[p, 0, n], stat_in[p, 1, n]) for p in range(blocks)])
    for tile in range(tiles):
        gathered(lambda p: stat_edge.at[p, tile], 1 + tile)
        for n, j in enumerate(edges):
            own = pl.ds(tile * PAD, PAD)
            mean_out[j, own, :], scale_out[j, own, :] = combine(
                [(stat_edge[p, tile, 0, n], stat_edge[p, tile, 1, n]) for p in range(blocks)]
            )


def write_kernel(far, mean, scale, anomaly_out, far_out, scaled, sems):
    planes, lines = far.shape[:2]
    halves = sems.shape[2]
    rows = lines // halves
    whole = [(j, pl.ds(h * rows, rows), h) for j in range(planes) for h in range(halves)]
    keep = [pltpu.make_async_copy(far.at[j, at], far_out.at[j, at], sems.at[0, j, h]) for j, at, h in whole]
    copies = [pltpu.make_async_copy(scaled.at[j, at], anomaly_out.at[j, at], sems.at[1, j, h]) for j, at, h in whole]
    for copy in keep:
        copy.start()
    for (j, at, h), copy in zip(whole, copies):
        middle, factor = mean[j], scale[j]

        def row(i, _, j=j, h=h, middle=middle, factor=factor):
            scaled[j, h * rows + i] = (far[j, h * rows + i] - middle) * factor
            return 0

        lax.fori_loop(0, rows, row, 0, unroll=8)
        copy.start()
    for copy in keep + copies:
        copy.wait()


def shards(jobs, pairs, axes, field_now, earlier, speed_square):
    planes, lines, depth, levels = shape = field_now.shape
    tiles = depth // PAD
    pieces = 1
    chunks = tiles * pieces
    rows = lines // pieces
    lent = rows // LENT if pairs and pieces == 1 and chunks >= 4 else 0
    end = rows // END if pieces == 1 and chunks >= 4 and (chunks % 2 == 0 or not jobs) else 0
    held = max([1] + [[v for _, _, v in jobs].count(via) for _, _, via in jobs])
    blocks = axes["px"]
    dma = pltpu.SemaphoreType.DMA
    f32 = jnp.float32
    middle = max(planes - 2, 1)
    edges = min(planes, 2)
    vmem = pl.BlockSpec(memory_space=pltpu.VMEM)
    anywhere = pl.BlockSpec(memory_space=pl.ANY)
    far, mean, scale = pl.pallas_call(
        functools.partial(steps_kernel, jobs, pieces, lent, end, axes),
        out_shape=[
            pltpu.VMEM(shape, f32),
            pltpu.VMEM((planes, depth, levels), f32),
            pltpu.VMEM((planes, depth, levels), f32),
        ],
        in_specs=[anywhere] * 3,
        out_specs=[vmem] * 3,
        scratch_shapes=[
            pltpu.VMEM((2, planes, lines + 2, depth + 2 * PAD, levels), f32),
            pltpu.VMEM(shape, f32),
            pltpu.VMEM((2, 2, lines, depth, levels), f32),
            pltpu.VMEM((held, STEPS, chunks // 2, rows, PAD, levels) if jobs else (1, 1, 1, 1, PAD, levels), f32),
            pltpu.VMEM((2, max(lent, 1), PAD, levels), f32),
            pltpu.VMEM((blocks, 2, middle, depth, levels), f32),
            pltpu.VMEM((blocks, tiles, 2, edges, PAD, levels), f32),
            dma((5,)),
            dma((2, 2, chunks)),
            dma((2, 2, chunks)),
            dma((held, STEPS, chunks // 2)),
            dma((held, STEPS, chunks // 2)),
            dma((2,)),
            dma((2,)),
            dma((2,)),
            dma((2, 2, 2)),
            dma((2, 2, 2)),
            dma((blocks, 1 + tiles)),
            dma((blocks, 1 + tiles)),
        ],
        compiler_params=pltpu.CompilerParams(
            collective_id=0, has_side_effects=True, vmem_limit_bytes=LIMIT,
        ),
    )(field_now, earlier, speed_square)
    anomaly, far = pl.pallas_call(
        write_kernel,
        out_shape=[jax.ShapeDtypeStruct(shape, f32)] * 2,
        in_specs=[vmem] * 3,
        out_specs=[anywhere] * 2,
        scratch_shapes=[pltpu.VMEM(shape, f32), dma((2, planes, 2))],
        compiler_params=pltpu.CompilerParams(vmem_limit_bytes=24 * 2**20),
    )(far, mean, scale)
    return (anomaly, far)


def solution(mesh):
    axes = dict(mesh.shape)
    return jax.shard_map(
        functools.partial(shards, relays(mesh), paired(mesh), axes),
        mesh=mesh,
        in_specs=(P("py", "px", "pz", None),) * 3,
        out_specs=(P("py", "px", "pz", None),) * 2,
        check_vma=False,
    )
```

```python
import functools

import jax
import jax.numpy as jnp
from jax import lax
from jax.experimental import pallas as pl
from jax.experimental.pallas import tpu as pltpu
from jax.sharding import PartitionSpec as P

STEPS = 4
PAD = 8
LENT = 4
END = 4
LIMIT = 54 * 2**20
MESH = pl.DeviceIdType.MESH


def relays(mesh):
    devices = mesh.devices
    line = [devices[(n,) + (0,) * (devices.ndim - 1)] for n in range(devices.shape[0])]
    places = [getattr(device, "coords", None) for device in line]
    if any(place is None for place in places):
        return ()
    places = [tuple(place) for place in places]
    jobs = []
    for low in range(len(line) - 1):
        for a, b in ((low, low + 1), (low + 1, low)):
            turn = (places[a][0],) + places[b][1:]
            if turn in places and turn not in (places[a], places[b]):
                jobs.append((a, b, places.index(turn)))
    return tuple(jobs)


def paired(mesh):
    row = mesh.devices[(0,) * (mesh.devices.ndim - 1)]
    places = [(getattr(device, "coords", None), getattr(device, "core_on_chip", None)) for device in row]
    if len(places) % 2 or any(None in place for place in places):
        return False
    twos = [(places[n], places[n + 1]) for n in range(0, len(places), 2)]
    return all(tuple(a[0]) == tuple(b[0]) and (a[1], b[1]) == (0, 1) for a, b in twos)


def steps_kernel(jobs, pieces, lent, end, axes, f_ref, e_ref, c_ref, far, mean_out, scale_out,
                 field, speed, halo, relay, lent_in, stat_in, stat_edge, load_sem, py_send, py_recv,
                 r_send, r_recv, lent_send, lent_recv, end_recv, side_send, side_recv, st_send, st_recv):
    planes, lines, depth, levels = c_ref.shape
    tiles = depth // PAD
    chunks = tiles * pieces
    rows = lines // pieces
    edges = sorted({0, planes - 1})
    inner = pl.ds(PAD, depth)
    me = {name: lax.axis_index(name) for name in axes}
    count = {name: axes[name] for name in axes}
    py = me["py"]

    staged = [
        pltpu.make_async_copy(f_ref.at[j, :, pl.ds(0, PAD)], far.at[j, :, pl.ds(0, PAD)], load_sem.at[3 + n])
        for n, j in enumerate(edges)
    ]
    for load in staged:
        load.start()

    barrier = pltpu.get_barrier_semaphore()
    greeted = 0
    met = sorted({(n, n + 1) for n in range(count["py"] - 1)} | {
        tuple(sorted(pair)) for a, b, via in jobs for pair in ((a, via), (via, b))
    })
    for low, high in met:
        for here, beyond in ((low, high), (high, low)):
            @pl.when(py == here)
            def _(beyond=beyond):
                pl.semaphore_signal(barrier, inc=1, device_id={"py": beyond}, device_id_type=MESH)
    known = sum((py == here).astype(jnp.int32) for pair in met for here in pair)
    for name in axes:
        if name == "py":
            continue
        for n in range(1, count[name]):
            pl.semaphore_signal(
                barrier, inc=1, device_id={name: lax.rem(me[name] + n, count[name])},
                device_id_type=MESH,
            )
            greeted += 1
    pl.semaphore_wait(barrier, known + greeted)

    def there(name, way):
        return me[name] < count[name] - 1 if way else me[name] > 0

    def done(ref, sem):
        pltpu.make_async_copy(ref, ref, sem).wait()

    def part(c, line, cell, held=(0, rows)):
        start = cell + (c // pieces) * PAD
        if cell % PAD == 0:
            start = pl.multiple_of(start, PAD)
        return pl.ds(line + (c % pieces) * rows + held[0], held[1]), pl.ds(start, PAD)

    def edge(step, c, way, held=(0, rows)):
        plane = planes - 1 if way else 0
        if step == 0:
            start = far if isinstance(c, int) else f_ref
            return start.at[(plane,) + part(c, 0, 0, held)]
        return field.at[(step % 2, plane) + part(c, 1, PAD, held)]

    def landing(step, c, side, held=(0, rows)):
        return halo.at[(side, step % 2) + part(c, 0, 0, held)]

    last = STEPS - 1
    own_part, lent_part = (0, rows - lent), (rows - lent, lent)
    head_part, end_part = (0, rows - end), (rows - end, end)
    mate = me["pz"] + 1 - 2 * lax.rem(me["pz"], 2)
    inner_core = lax.rem(me["pz"], 2) == 0

    def shares(way):
        busy = there("py", way)
        for a, b, _ in jobs:
            if b - a != 2 * way - 1:
                busy = jnp.logical_and(busy, py != a)
        return busy

    def pass_lent(c):
        if lent:
            for way in (0, 1):
                @pl.when(jnp.logical_and(jnp.logical_and(c == 2, jnp.logical_not(inner_core)), shares(way)))
                def _(way=way):
                    done(lent_in.at[way], lent_recv.at[way])
                    pltpu.make_async_remote_copy(
                        src_ref=lent_in.at[way],
                        dst_ref=landing(last, 1, 1 - way, lent_part),
                        send_sem=lent_send.at[way],
                        recv_sem=py_recv.at[1 - way, last % 2, 1],
                        device_id={"py": py + (2 * way - 1), "pz": mate}, device_id_type=MESH,
                    ).start()

    def send_py(step, c):
        for way in (0, 1):
            beyond = py + (2 * way - 1)
            direct = there("py", way)
            for slot, (a, b, via) in enumerate(jobs):
                if b - a != 2 * way - 1:
                    continue
                turned = jnp.logical_and(py == a, jnp.int32(c) % 2 == 0)
                direct = jnp.logical_and(direct, jnp.logical_not(turned))

                @pl.when(turned)
                def _(slot=slot, via=via, way=way):
                    pltpu.make_async_remote_copy(
                        src_ref=edge(step, c, way),
                        dst_ref=relay.at[job_slot(slot), step, c // 2],
                        send_sem=py_send.at[way, step % 2, c],
                        recv_sem=r_recv.at[job_slot(slot), step, c // 2],
                        device_id={"py": via}, device_id_type=MESH,
                    ).start()

            if lent and step == last:
                split = jnp.logical_and(jnp.logical_and(c == 1, inner_core), jnp.logical_and(direct, shares(way)))
                direct = jnp.logical_and(direct, jnp.logical_not(split))

                @pl.when(split)
                def _(way=way, beyond=beyond):
                    pltpu.make_async_remote_copy(
                        src_ref=edge(step, c, way, lent_part),
                        dst_ref=lent_in.at[way],
                        send_sem=py_send.at[way, step % 2, c],
                        recv_sem=lent_recv.at[way],
                        device_id={"pz": mate}, device_id_type=MESH,
                    ).start()
                    pltpu.make_async_remote_copy(
                        src_ref=edge(step, c, way, own_part),
                        dst_ref=landing(step, c, 1 - way, own_part),
                        send_sem=py_send.at[way, step % 2, c],
                        recv_sem=py_recv.at[1 - way, step % 2, c],
                        device_id={"py": beyond}, device_id_type=MESH,
                    ).start()

            if end and step == last:
                ends = jnp.logical_and(direct, c == chunks - 1)
                direct = jnp.logical_and(direct, c != chunks - 1)

                @pl.when(ends)
                def _(way=way, beyond=beyond):
                    for held, sem in ((head_part, py_recv.at[1 - way, step % 2, c]), (end_part, end_recv.at[1 - way])):
                        pltpu.make_async_remote_copy(
                            src_ref=edge(step, c, way, held),
                            dst_ref=landing(step, c, 1 - way, held),
                            send_sem=py_send.at[way, step % 2, c],
                            recv_sem=sem,
                            device_id={"py": beyond}, device_id_type=MESH,
                        ).start()

            @pl.when(direct)
            def _(way=way, beyond=beyond):
                pltpu.make_async_remote_copy(
                    src_ref=edge(step, c, way),
                    dst_ref=landing(step, c, 1 - way),
                    send_sem=py_send.at[way, step % 2, c],
                    recv_sem=py_recv.at[1 - way, step % 2, c],
                    device_id={"py": beyond}, device_id_type=MESH,
                ).start()

    def job_slot(slot):
        return [via for _, _, via in jobs[:slot]].count(jobs[slot][2])

    def forward(step, c):
        for slot, (a, b, via) in enumerate(jobs):
            @pl.when(py == via)
            def _(slot=slot, a=a, b=b):
                way = 1 if b > a else 0
                held = relay.at[job_slot(slot), step, c // 2]
                done(held, r_recv.at[job_slot(slot), step, c // 2])
                pltpu.make_async_remote_copy(
                    src_ref=held,
                    dst_ref=landing(step, c, 1 - way),
                    send_sem=r_send.at[job_slot(slot), step, c // 2],
                    recv_sem=py_recv.at[1 - way, step % 2, c],
                    device_id={"py": b}, device_id_type=MESH,
                ).start()

    def forward_late(step, c):
        if jobs and not isinstance(c, int):
            @pl.when(c % 2 == 1)
            def _():
                forward(step, c - 1)

    def sent_py(step, c):
        for way in (0, 1):
            @pl.when(there("py", way))
            def _(way=way):
                done(edge(step, c, way), py_send.at[way, step % 2, c])

    def arrived_py(step, c):
        for side in (0, 1):
            @pl.when(there("py", side))
            def _(side=side):
                done(landing(step, c, side), py_recv.at[side, step % 2, c])

    def side_source(step, name, way):
        if name == "px":
            at = lines - 1 if way else 0
            if step == 0:
                return f_ref.at[:, pl.ds(at, 1)]
            return field.at[step % 2, :, pl.ds(1 + at, 1), inner]
        at = depth - PAD if way else 0
        if step == 0:
            return f_ref.at[:, :, pl.ds(at, PAD)]
        return field.at[step % 2, :, pl.ds(1, lines), pl.ds(PAD + at, PAD)]

    def side_landing(slot, name, side):
        if name == "px":
            return field.at[slot, :, pl.ds(lines + 1 if side else 0, 1), inner]
        return field.at[slot, :, pl.ds(1, lines), pl.ds(PAD + depth if side else 0, PAD)]

    def sides(step, what):
        for n, name in enumerate(("px", "pz")):
            for way in (0, 1):
                @pl.when(there(name, way))
                def _(n=n, name=name, way=way):
                    if what == "send":
                        pltpu.make_async_remote_copy(
                            src_ref=side_source(step, name, way),
                            dst_ref=side_landing(step % 2, name, 1 - way),
                            send_sem=side_send.at[n, way, step % 2],
                            recv_sem=side_recv.at[n, 1 - way, step % 2],
                            device_id={name: me[name] + (2 * way - 1)}, device_id_type=MESH,
                        ).start()
                    elif what == "sent":
                        done(side_source(step, name, way), side_send.at[n, way, step % 2])
                    else:
                        done(side_landing(step % 2, name, way), side_recv.at[n, way, step % 2])

    whole = lambda slot: field.at[slot, :, pl.ds(1, lines), inner]
    loads = [
        pltpu.make_async_copy(f_ref, whole(0), load_sem.at[0]),
        pltpu.make_async_copy(e_ref, whole(1), load_sem.at[1]),
        pltpu.make_async_copy(c_ref, speed, load_sem.at[2]),
    ]

    def first(c, _):
        send_py(0, c)
        forward_late(0, c)
        return 0

    for load in staged:
        load.wait()
    first(0, 0)
    first(jnp.int32(1), 0)
    sides(0, "send")
    for load in loads:
        load.start()
    lax.fori_loop(2, chunks, first, 0)

    for way in (0, 1):
        @pl.when(jnp.logical_not(there("py", way)))
        def _(way=way):
            def clear(i, _):
                for slot in (0, 1):
                    halo[way, slot, i] = jnp.zeros((depth, levels), jnp.float32)
                return 0
            lax.fori_loop(0, lines, clear, 0)

        @pl.when(jnp.logical_not(there("px", way)))
        def _(way=way):
            for slot in (0, 1):
                for j in range(planes):
                    field[slot, j, lines + 1 if way else 0, inner, :] = jnp.zeros((depth, levels), jnp.float32)

        @pl.when(jnp.logical_not(there("pz", way)))
        def _(way=way):
            def clear(i, _):
                for slot in (0, 1):
                    for j in range(planes):
                        field[slot, j, 1 + i, pl.ds(PAD + depth if way else 0, PAD), :] = jnp.zeros((PAD, levels), jnp.float32)
                return 0
            lax.fori_loop(0, lines, clear, 0)

    for load in loads:
        load.wait()

    px, blocks = me["px"], count["px"]

    def cells(start, tile):
        start = start + tile * PAD
        return pl.ds(pl.multiple_of(start, PAD) if isinstance(start, jax.Array) and start.ndim == 0 else start, PAD)

    def update(step, which, i, tile):
        now, other = step % 2, (step + 1) % 2
        mid, own = cells(PAD, tile), cells(0, tile)
        for j in which:
            here = field[now, j, i + 1, mid, :]
            below = field[now, j - 1, i + 1, mid, :] if j else halo[0, now, i, own, :]
            above = field[now, j + 1, i + 1, mid, :] if j < planes - 1 else halo[1, now, i, own, :]
            spread = (
                below + above
                + field[now, j, i, mid, :] + field[now, j, i + 2, mid, :]
                + field[now, j, i + 1, pl.ds(PAD - 1 + tile * PAD, PAD), :]
                + field[now, j, i + 1, pl.ds(PAD + 1 + tile * PAD, PAD), :]
                - 6.0 * here
            )
            later = 2.0 * here - field[other, j, i + 1, mid, :] + speed[j, i, own, :] * spread
            if step < STEPS - 1:
                field[other, j, i + 1, mid, :] = later
            else:
                far[j, i, own, :] = later

    def sums(which, tile, held=None, first=0, stop=lines):
        own = cells(0, tile)
        base = [far[j, 0, own, :] for j in which]

        def add(i, held):
            moved = [far[j, i, own, :] - b for j, b in zip(which, base)]
            return [(t + m, q + m * m) for (t, q), m in zip(held, moved)]

        zero = jnp.zeros((PAD, levels), jnp.float32)
        held = [(zero, zero) for _ in which] if held is None else held
        held = lax.fori_loop(first, stop, add, held, unroll=8)
        return held if stop < lines else [
            (b + t / lines, jnp.maximum(q - t * (t / lines), 0.0)) for b, (t, q) in zip(base, held)
        ]

    def send_stat(ref, slot):
        for n in range(blocks - 1, 0, -1):
            for way in (0, 1):
                to = px + n if way else px - n

                @pl.when(to < blocks if way else to >= 0)
                def _(n=n, way=way, to=to):
                    pltpu.make_async_remote_copy(
                        src_ref=ref, dst_ref=ref,
                        send_sem=st_send.at[n if way else blocks - n, slot], recv_sem=st_recv.at[px, slot],
                        device_id={"px": to}, device_id_type=MESH,
                    ).start()

    def edge_stat(tile, found):
        for n, (mean, squares) in enumerate(found):
            stat_edge[px, tile, 0, n] = mean
            stat_edge[px, tile, 1, n] = squares
        send_stat(stat_edge.at[px, tile], 1 + tile)
        return 0

    for step in range(STEPS):
        now, other = step % 2, (step + 1) % 2
        sides(step, "arrived")
        if step >= 1:
            sides(step - 1, "sent")

        which = range(planes)
        if step == STEPS - 1:
            which = edges
            if planes > 2:
                def middle(tile, _):
                    def row(i, _):
                        update(STEPS - 1, range(1, planes - 1), i, tile)
                        return 0

                    lax.fori_loop(0, lines, row, 0, unroll=4)
                    for n, (mean, squares) in enumerate(sums(range(1, planes - 1), tile)):
                        stat_in[px, 0, n, cells(0, tile), :] = mean
                        stat_in[px, 1, n, cells(0, tile), :] = squares
                    return 0

                lax.fori_loop(0, tiles, middle, 0)
                send_stat(stat_in.at[px], 0)

        def chunk(c, _, step=step, which=which):
            arrived_py(step, c)
            if step >= 1:
                sent_py(step - 1, c)
            tile, first_line = c // pieces, (c % pieces) * rows

            def row(r, _):
                update(step, which, first_line + r, tile)
                return 0

            lax.fori_loop(0, rows, row, 0, unroll=4)
            if step < STEPS - 1:
                forward_late(step + 1, c)
                send_py(step + 1, c)
                if step + 1 == last:
                    pass_lent(c)
            else:
                @pl.when(c % pieces == pieces - 1)
                def _():
                    edge_stat(tile, sums(edges, tile))
            return 0

        lax.fori_loop(0, chunks - 1 if end and step == last else chunks, chunk, 0)
        if end and step == last:
            c, held = chunks - 1, None
            sent_py(step - 1, c)
            for first, n in (head_part, end_part):
                for side in (0, 1):
                    @pl.when(there("py", side))
                    def _(side=side, first=first, n=n):
                        arrival = py_recv.at[side, last % 2, c] if first == 0 else end_recv.at[side]
                        done(landing(last, c, side, (first, n)), arrival)

                def row(r, _):
                    update(step, edges, r, c)
                    return 0

                lax.fori_loop(first, first + n, row, 0, unroll=8)
                held = sums(edges, c, held, first, first + n)
            edge_stat(c, held)
        if step < STEPS - 1:
            sides(step + 1, "send")

    def settle(c, _):
        sent_py(STEPS - 1, c)
        return 0

    lax.fori_loop(0, chunks, settle, 0)
    sides(STEPS - 1, "sent")
    for slot, (_, _, via) in enumerate(jobs):
        @pl.when(py == via)
        def _(slot=slot):
            for step in range(STEPS):
                for c in range(chunks // 2):
                    done(relay.at[job_slot(slot), step, c], r_send.at[job_slot(slot), step, c])

    if lent:
        for way in (0, 1):
            @pl.when(jnp.logical_and(jnp.logical_not(inner_core), shares(way)))
            def _(way=way):
                done(lent_in.at[way], lent_send.at[way])

    def combine(parts):
        mean = parts[0][0]
        for m, _ in parts[1:]:
            mean = mean + m
        mean = mean / blocks
        squares = jnp.zeros_like(mean)
        for m, q in parts:
            off = m - mean
            squares = squares + (q + lines * (off * off))
        return mean, lax.rsqrt(squares / (lines * blocks) + 0.0001)

    def gathered(at, slot):
        for n in range(1, blocks):
            source = lax.rem(px + n, blocks)
            done(at(px), st_send.at[n, slot])
            done(at(source), st_recv.at[source, slot])

    if planes > 2:
        gathered(lambda p: stat_in.at[p], 0)
        for n in range(planes - 2):
            mean_out[1 + n], scale_out[1 + n] = combine([(stat_in[p, 0, n], stat_in[p, 1, n]) for p in range(blocks)])
    for tile in range(tiles):
        gathered(lambda p: stat_edge.at[p, tile], 1 + tile)
        for n, j in enumerate(edges):
            own = pl.ds(tile * PAD, PAD)
            mean_out[j, own, :], scale_out[j, own, :] = combine(
                [(stat_edge[p, tile, 0, n], stat_edge[p, tile, 1, n]) for p in range(blocks)]
            )


def write_kernel(far, mean, scale, anomaly_out, far_out, scaled, sems):
    planes, lines = far.shape[:2]
    halves = sems.shape[2]
    rows = lines // halves
    whole = [(j, pl.ds(h * rows, rows), h) for j in range(planes) for h in range(halves)]
    keep = [pltpu.make_async_copy(far.at[j, at], far_out.at[j, at], sems.at[0, j, h]) for j, at, h in whole]
    copies = [pltpu.make_async_copy(scaled.at[j, at], anomaly_out.at[j, at], sems.at[1, j, h]) for j, at, h in whole]
    for copy in keep:
        copy.start()
    for (j, at, h), copy in zip(whole, copies):
        middle, factor = mean[j], scale[j]

        def row(i, _, j=j, h=h, middle=middle, factor=factor):
            scaled[j, h * rows + i] = (far[j, h * rows + i] - middle) * factor
            return 0

        lax.fori_loop(0, rows, row, 0, unroll=8)
        copy.start()
    for copy in keep + copies:
        copy.wait()


def shards(jobs, pairs, axes, field_now, earlier, speed_square):
    planes, lines, depth, levels = shape = field_now.shape
    tiles = depth // PAD
    pieces = 1
    chunks = tiles * pieces
    rows = lines // pieces
    lent = rows // LENT if pairs and pieces == 1 and chunks >= 4 else 0
    end = rows // END if pieces == 1 and chunks >= 4 and (chunks % 2 == 0 or not jobs) else 0
    held = max([1] + [[v for _, _, v in jobs].count(via) for _, _, via in jobs])
    blocks = axes["px"]
    dma = pltpu.SemaphoreType.DMA
    f32 = jnp.float32
    middle = max(planes - 2, 1)
    edges = min(planes, 2)
    vmem = pl.BlockSpec(memory_space=pltpu.VMEM)
    anywhere = pl.BlockSpec(memory_space=pl.ANY)
    far, mean, scale = pl.pallas_call(
        functools.partial(steps_kernel, jobs, pieces, lent, end, axes),
        out_shape=[
            pltpu.VMEM(shape, f32),
            pltpu.VMEM((planes, depth, levels), f32),
            pltpu.VMEM((planes, depth, levels), f32),
        ],
        in_specs=[anywhere] * 3,
        out_specs=[vmem] * 3,
        scratch_shapes=[
            pltpu.VMEM((2, planes, lines + 2, depth + 2 * PAD, levels), f32),
            pltpu.VMEM(shape, f32),
            pltpu.VMEM((2, 2, lines, depth, levels), f32),
            pltpu.VMEM((held, STEPS, chunks // 2, rows, PAD, levels) if jobs else (1, 1, 1, 1, PAD, levels), f32),
            pltpu.VMEM((2, max(lent, 1), PAD, levels), f32),
            pltpu.VMEM((blocks, 2, middle, depth, levels), f32),
            pltpu.VMEM((blocks, tiles, 2, edges, PAD, levels), f32),
            dma((5,)),
            dma((2, 2, chunks)),
            dma((2, 2, chunks)),
            dma((held, STEPS, chunks // 2)),
            dma((held, STEPS, chunks // 2)),
            dma((2,)),
            dma((2,)),
            dma((2,)),
            dma((2, 2, 2)),
            dma((2, 2, 2)),
            dma((blocks, 1 + tiles)),
            dma((blocks, 1 + tiles)),
        ],
        compiler_params=pltpu.CompilerParams(
            collective_id=0, has_side_effects=True, vmem_limit_bytes=LIMIT,
        ),
    )(field_now, earlier, speed_square)
    anomaly, far = pl.pallas_call(
        write_kernel,
        out_shape=[jax.ShapeDtypeStruct(shape, f32)] * 2,
        in_specs=[vmem] * 3,
        out_specs=[anywhere] * 2,
        scratch_shapes=[pltpu.VMEM(shape, f32), dma((2, planes, 1))],
        compiler_params=pltpu.CompilerParams(vmem_limit_bytes=24 * 2**20),
    )(far, mean, scale)
    return (anomaly, far)


def solution(mesh):
    axes = dict(mesh.shape)
    return jax.shard_map(
        functools.partial(shards, relays(mesh), paired(mesh), axes),
        mesh=mesh,
        in_specs=(P("py", "px", "pz", None),) * 3,
        out_specs=(P("py", "px", "pz", None),) * 2,
        check_vma=False,
    )
```
